512 devices in a mesh: parts: 2 (over y), gz: 128 (over x, z), gy: 2 (over core).
Axes of the slice: x: 8, y: 2, z: 16, core: 2. Of those that a mesh axis runs over, the one named last changes fastest.
The devices are a block of a 8x8x16 slice.
Arguments:
- direction: float32 [3, 256, 128, 128], P(None, ('parts', 'gz'), 'gy'), parts along dimension 1, may hold values from -6 to 6
- region: int32 [256, 128, 128], P(('parts', 'gz'), 'gy'), parts along dimension 0, may hold values from 0 to 3
- saturation: float32 [3], replicated, may hold values from 0.5 to 2
- kernel_main: float32 [6, 256, 256, 128], P(None, 'gz', 'gy'), may hold values from -6 to 6
- kernel_nyq: float32 [6, 256, 256], P(None, 'gz', 'gy'), may hold values from -6 to 6
Outputs:
- field: float32 [3, 256, 128, 128], P(None, ('parts', 'gz'), 'gy'), parts along dimension 1
The draws below stay inside these ranges and needn't reach their ends.
There are 2 independent parts, one for each index of `parts`. The reference program is written for one: setup_inputs(seed, part) draws one part's arguments, and reference() takes and returns one part's arrays. A program takes and returns all parts, laid end to end along the dimension named above; an argument that names none is the same for every part. Nothing has to cross between parts.
Inputs may be any that keep to these rules, and one draw needn't show every extreme that they name: `region`: 0 marks an empty cell; other ids name materials.
All inputs are finite; a program needn't handle non-finite values.
Results may differ from the reference program's by a relative error of at most 0.00007.
Values sent between devices are 32-bit elements; how exact they have to be, the bound alone decides.
No kernel may reach another device: no remote copies, remote signals or barrier semaphores. Data moves between devices by JAX's collectives and lax.ppermute only.
A program may use at most 64 MiB of HBM per device.

```python
import math
import jax
import jax.numpy as jnp
import numpy as np

MX = 128
MY = 128
REGIONS = 4
MZ = 128
PY = 256
PZ = 256
ZBITS = 7


def touch_ends(array, key, smallest, largest):
    place = [jax.random.randint(jax.random.fold_in(key, axis), (), 0, length) for axis, length in enumerate(array.shape)]
    longest = array.shape.index(max(array.shape))
    neighbour = place[:longest] + [(place[longest] + 1) % array.shape[longest]] + place[longest + 1:]
    return array.at[tuple(place)].set(smallest).at[tuple(neighbour)].set(largest)


def level_of(own_key, dims, cuts, least, high):
    loudness, own = 1.0, jax.random.fold_in(own_key, 6)
    for dim, shards_of in cuts:
        draws = jnp.exp(jax.random.uniform(jax.random.fold_in(own, dim), (shards_of,), jnp.float32, least / len(cuts), high / len(cuts)))
        loudness = loudness * jnp.repeat(draws, dims[dim] // shards_of).reshape([-1 if axis == dim else 1 for axis in range(len(dims))])
    return loudness


def noise(rng, extent, deviation, reach, cuts=(), dtype=jnp.bfloat16):
    entries = jax.random.normal(rng, extent, jnp.float32) * deviation
    if len(cuts) > 0:
        entries = level_of(rng, extent, cuts, -0.22, 0.18) * entries
    return jnp.clip(entries, min=-reach, max=reach).astype(dtype)


def setup_inputs(seed: int = 0, part: int = 0) -> dict:
    seeds = jax.random.split(jax.random.key(seed), 6)
    part_keys = jax.random.split(jax.random.fold_in(seeds[5], part), 6)
    return {
        "direction": noise(part_keys[0], (3, MZ, MY, MX), 1.0, 6.0, ((1, 128), (2, 2)), jnp.float32),
        "region": touch_ends(jax.random.randint(part_keys[1], (MZ, MY, MX), 0, REGIONS), jax.random.fold_in(part_keys[1], 1), 0, REGIONS - 1).astype(jnp.int32),
        "saturation": jnp.clip(jnp.exp(jax.random.uniform(seeds[2], (REGIONS - 1,), jnp.float32, math.log(0.5), math.log(2.0))), 0.5, 2.0),
        "kernel_main": noise(seeds[3], (6, PZ, PY, MX), 1.0, 6.0, ((1, 128), (2, 2)), jnp.float32),
        "kernel_nyq": noise(seeds[4], (6, PZ, PY), 1.0, 6.0, ((1, 128), (2, 2)), jnp.float32),
    }


exchange_stiffness = 0.25
tensor_index = ((0, 3, 4), (3, 1, 5), (4, 5, 2))


def slot_order(bit_count):
    slot_index = np.arange(2 ** (bit_count + 1))
    device = slot_index // 2
    reversed_bits = device * 0
    for b in range(bit_count):
        reversed_bits = reversed_bits + ((device >> b) & 1) * (2 ** (bit_count - 1 - b))
    return 2 * reversed_bits + slot_index % 2


def neighbours(padded):
    summed = padded[..., 2:, 1:-1, 1:-1] + padded[..., :-2, 1:-1, 1:-1]
    summed = summed + padded[..., 1:-1, 2:, 1:-1] + padded[..., 1:-1, :-2, 1:-1]
    return summed + padded[..., 1:-1, 1:-1, 2:] + padded[..., 1:-1, 1:-1, :-2]


def reference(direction, region, saturation, kernel_main, kernel_nyq):
    magnetic = (region > 0).astype(jnp.float32)
    strength = jnp.zeros(region.shape, jnp.float32)
    for r in range(REGIONS - 1):
        strength = strength + jnp.where(region == r + 1, saturation[r], 0.0)
    moment = direction * strength[None]
    padded = jnp.zeros((3, 2 * MZ, 2 * MY, 2 * MX), jnp.float32).at[:, :MZ, :MY, :MX].set(moment)
    spectra = jnp.fft.rfftn(padded, axes=(1, 2, 3))
    inverse_slots = np.argsort(slot_order(ZBITS)).astype(np.int32)
    kernel = jnp.concatenate([kernel_main, kernel_nyq[..., None]], axis=3)[:, inverse_slots]
    pieces = []
    for i in range(3):
        summed = kernel[tensor_index[i][0]] * spectra[0]
        for j in (1, 2):
            summed = summed + kernel[tensor_index[i][j]] * spectra[j]
        pieces.append(summed)
    demag = jnp.fft.irfftn(jnp.stack(pieces), s=(2 * MZ, 2 * MY, 2 * MX), axes=(1, 2, 3))
    demag = demag[:, :MZ, :MY, :MX]
    moment_rim = jnp.pad(direction * magnetic[None], ((0, 0), (1, 1), (1, 1), (1, 1)))
    count_rim = jnp.pad(magnetic, 1)
    near = neighbours(moment_rim)
    count = neighbours(count_rim)
    exchange = exchange_stiffness * magnetic[None] * (near - count[None] * direction)
    return (demag + exchange).astype(jnp.float32)
```

```python
import math

import jax
import jax.numpy as jnp
import numpy as np
from jax import lax
from jax.sharding import PartitionSpec as P

exchange_stiffness = 0.25
tensor_index = ((0, 3, 4), (3, 1, 5), (4, 5, 2))
highest = lax.Precision.HIGHEST
lane_width = 128
swap = [(0, 1), (1, 0)]


def wave(first, second, period):
    angle = 2.0 * np.pi / period * (np.outer(first, second) % period)
    return np.cos(angle), np.sin(angle)


def slot_frequencies(groups_z):
    bits = groups_z.bit_length() - 1
    reversed_bits = np.array([int(format(d, f"0{bits}b")[::-1], 2) for d in range(groups_z)])
    return np.concatenate([2 * reversed_bits, 2 * reversed_bits + 1])


def tables(columns, rows, groups_z):
    f32 = lambda a: np.ascontiguousarray(a, dtype=np.float32)
    x = np.arange(columns)
    y = np.arange(rows)
    ky = np.arange(2 * rows)
    z = np.arange(groups_z)
    out = {}
    cx, sx = wave(x, x, 2 * columns)
    out["tx"] = f32(np.concatenate([cx, -sx], axis=1))
    half = rows // 2
    per_gy, per_gy_back = [], []
    for g in range(2):
        own_ky = ky[g * rows : (g + 1) * rows]
        blocks = []
        for h in (g, 1 - g):
            c, s = wave(y[h * half : (h + 1) * half], own_ky, 2 * rows)
            blocks.append(np.block([[c, -s], [s, c]]))
        per_gy.append(np.concatenate(blocks, axis=0))
        blocks = []
        for h in (g, 1 - g):
            c, s = wave(own_ky, y[h * half : (h + 1) * half], 2 * rows)
            blocks.append(np.block([[c, s], [-s, c]]))
        per_gy_back.append(np.concatenate(blocks, axis=1))
    out["ty"] = f32(np.stack(per_gy))
    out["ty_back"] = f32(np.stack(per_gy_back))
    kz = slot_frequencies(groups_z)
    c, s = wave(kz, z, 2 * groups_z)
    out["tz"] = f32(np.concatenate([c, s], axis=1))
    out["tz_back"] = f32(np.concatenate([c.T, s.T], axis=1))
    w = np.where(x == 0, 1.0, 2.0)[:, None]
    scale = 1.0 / (2.0 * columns * 2.0 * rows * 2.0 * groups_z)
    out["tx_back"] = f32(np.concatenate([w * cx, -w * sx], axis=1) * scale)
    forward, back = [], []
    for g in range(2):
        c, s = wave(ky[g * rows : (g + 1) * rows], np.concatenate([y[g * half : (g + 1) * half], y[(1 - g) * half : (2 - g) * half]]), 2 * rows)
        forward.append(np.stack([c, -s]))
        c, s = wave(ky, y[g * half : (g + 1) * half], 2 * rows)
        c, s = c.reshape(2, rows, half), s.reshape(2, rows, half)
        back.append(np.stack([c[0], -s[0], c[1], -s[1]]) * scale)
    out["ny"] = f32(np.stack(forward))
    out["ny_back"] = f32(np.stack(back))
    return {k: jnp.asarray(v) for k, v in out.items()}


def dot(a, b):
    return jnp.dot(a, b, precision=highest)


def spread(values):
    rows = values.shape[0]
    one = jnp.pad(values, ((0, 0), (0, 1)))
    return jnp.pad(jnp.concatenate([one, one, one], axis=1), ((0, 0), (0, 20)))


def spread_kernel(kernel):
    rows = [kernel[tensor_index[i][j]] if i < 3 and j < 3 else jnp.zeros_like(kernel[0]) for i in range(4) for j in range(4)]
    return jnp.stack(rows, axis=1)


def forward_x(moment, tx):
    three, rows, columns = moment.shape
    table = tx.reshape(columns, 2, columns)
    out = jnp.einsum("krx,cyx->kcry", table, moment, precision=highest)
    return out.reshape(columns, three, 2 * rows)


def forward_yz(own, other, ty, tz):
    both = jnp.concatenate([own, other], axis=2)
    planes, three, width = both.shape
    ready = dot(both.reshape(planes * three, width), ty).reshape(planes, three, 2, -1)
    real = ready[:, :, 0].transpose(1, 0, 2)
    imag = ready[:, :, 1].transpose(1, 0, 2)
    to_real = jnp.concatenate([real, imag], axis=1)
    to_imag = jnp.concatenate([imag, -real], axis=1)
    return jnp.stack(
        [
            jnp.einsum("pq,cqk->cpk", tz, to_real, precision=highest),
            jnp.einsum("pq,cqk->cpk", tz, to_imag, precision=highest),
        ],
        axis=1,
    )


def multiply_back(spectra, kernel, extra, tz, tz_back, ty_back, y_index):
    kernel = kernel.reshape(6, -1, kernel.shape[2])
    pieces = []
    for i in range(3):
        summed = kernel[tensor_index[i][0]] * spectra[0]
        for j in (1, 2):
            summed = summed + kernel[tensor_index[i][j]] * spectra[j]
        pieces.append(summed)
    field = jnp.stack(pieces)
    to_real = jnp.concatenate([field[:, 0], -field[:, 1]], axis=1)
    to_imag = jnp.concatenate([field[:, 1], field[:, 0]], axis=1)
    real = jnp.einsum("zp,cpk->czk", tz_back, to_real, precision=highest)
    imag = jnp.einsum("zp,cpk->czk", tz_back, to_imag, precision=highest)
    lines = jnp.concatenate([real, imag], axis=2)
    both = jnp.einsum("czk,ky->zcy", lines, ty_back, precision=highest)
    real, imag = extra[:, 0:12], extra[:, 32:44]
    k_col = jnp.concatenate([extra[:, 16:28], extra[:, 80:92]], axis=0)
    z_real = dot(tz, jnp.concatenate([real, imag], axis=0)) * k_col
    z_imag = dot(tz, jnp.concatenate([imag, -real], axis=0)) * k_col
    q_real = dot(tz_back, jnp.concatenate([z_real, -z_imag], axis=0))
    q_imag = dot(tz_back, jnp.concatenate([z_imag, z_real], axis=0))
    row = jnp.concatenate([jnp.pad(q_real, ((0, 0), (0, 20))), jnp.pad(q_imag, ((0, 0), (0, 20)))], axis=1)
    zero = jnp.zeros_like(row)
    row = jnp.concatenate([jnp.where(y_index == 0, row, zero), jnp.where(y_index == 1, row, zero)], axis=1)
    half = both.shape[2] // 2
    return (
        jnp.concatenate([both[:, :, :half], row[:, None]], axis=1),
        jnp.concatenate([both[:, :, half:], row[:, None]], axis=1),
    )


def back_x(received, tx_back, ny_back, signs):
    columns = received.shape[0]
    half = received.shape[2] // 2
    main = received[:, :3].reshape(columns, 3, 2, half)
    table = tx_back.reshape(columns, 2, columns)
    demag = jnp.einsum("kcry,krx->cyx", main, table, precision=highest)
    extra = received[:, 3].reshape(columns, 4, 32)[:, :, :12].reshape(columns, 4, 3, 4)[..., :3].sum(axis=3)
    nyquist = jnp.einsum("gqi,qgy->iy", extra, ny_back, precision=highest)
    return demag + nyquist[:, :, None] * signs


def local(direction, region, saturation, kernel_main, kernel_nyq):
    columns = direction.shape[3]
    half = direction.shape[2]
    groups_z = lax.axis_size("gz")
    rows = half * lax.axis_size("gy")
    y_index = lax.axis_index("gy")
    t = tables(columns, rows, groups_z)
    direction = direction[:, 0]
    region = region[0]
    magnetic = (region > 0).astype(jnp.float32)
    strength = jnp.zeros(region.shape, jnp.float32)
    for r in range(saturation.shape[0]):
        strength = strength + jnp.where(region == r + 1, saturation[r], 0.0)
    moment = direction * strength[None]
    signs = (1.0 - 2.0 * (jnp.arange(columns) % 2)).astype(jnp.float32)
    stacked = jnp.concatenate([direction * magnetic[None], magnetic[None]], axis=0)
    parts = lax.axis_size("parts")
    part = lax.axis_index("parts")
    share = -(-12 // parts)
    nyq_own = jnp.sum(moment * signs, axis=2)
    edge = jnp.where(y_index == 0, stacked[:, -1], stacked[:, 0])
    small = jnp.concatenate([edge, jnp.pad(nyq_own, ((0, 1), (0, columns - half)))], axis=0)
    small = lax.ppermute(small, "gy", swap)
    edge, nyq_other = small[:4], small[4:7, :half]
    line = jnp.concatenate([nyq_own, nyq_other], axis=1)
    nyq = jnp.einsum("rgy,cy->rgc", t["ny"][y_index], line, precision=highest)
    k_row = [spread_kernel(kernel_nyq[:, s]) for s in range(2)]
    zero = jnp.zeros_like(k_row[0])
    real, imag = spread(nyq[0]), spread(nyq[1])
    row = jnp.concatenate(
        [real[:, :16], k_row[0], imag[:, :16], zero, zero, k_row[1], zero, zero], axis=1
    )
    mine = jnp.minimum(part * share, 12 - share)
    main = lax.dynamic_slice_in_dim(kernel_main.reshape(12, rows, columns), mine, share, 0)
    send = jnp.concatenate([forward_x(moment, t["tx"]), row[:, None], main.transpose(2, 0, 1)], axis=1)
    width = send.shape[1]
    recv = lax.all_to_all(send.reshape(columns, width // 2, 2, columns), "gz", 0, 0, tiled=True)
    recv = recv.reshape(columns, width, columns)
    recv_m, recv_n, recv_k = recv[:, :3], recv[:, 3], recv[:, 4:]
    other_m = lax.ppermute(recv_m, "gy", swap)
    shares = [recv_k]
    for k in range(1, parts):
        shares.append(lax.ppermute(recv_k, "parts", [(p, (p + k) % parts) for p in range(parts)]))
    ordered = []
    for c in range(12):
        owner = c // share
        at = c - min(owner * share, 12 - share)
        piece = shares[0][:, at]
        for k in range(1, parts):
            piece = jnp.where((part - owner) % parts == k, shares[k][:, at], piece)
        ordered.append(piece)
    kernel = jnp.stack(ordered)
    up = [(i, i + 1) for i in range(groups_z - 1)]
    down = [(b, a) for a, b in up]
    before = lax.ppermute(stacked, "gz", up)
    after = lax.ppermute(stacked, "gz", down)
    spectra = forward_yz(recv_m, other_m, t["ty"][y_index], t["tz"])
    own, other = multiply_back(spectra, kernel, recv_n, t["tz"], t["tz_back"], t["ty_back"][y_index], y_index)
    send_f = own + lax.ppermute(other, "gy", swap)
    recv_f = lax.all_to_all(send_f, "gz", 0, 0, tiled=True)
    demag = back_x(recv_f, t["tx_back"], t["ny_back"][y_index], signs)
    low = jnp.where(y_index == 0, 0.0, edge)[:, None]
    high = jnp.where(y_index == 0, edge, 0.0)[:, None]
    tall = jnp.concatenate([low, stacked, high], axis=1)
    wide = jnp.pad(stacked, ((0, 0), (0, 0), (1, 1)))
    near = before + after + tall[:, :-2] + tall[:, 2:] + wide[..., :-2] + wide[..., 2:]
    exchange = exchange_stiffness * magnetic[None] * (near[:3] - near[3:4] * direction)
    return (demag + exchange)[:, None]


def solution(mesh):
    placed = (
        P(None, ("parts", "gz"), "gy", None),
        P(("parts", "gz"), "gy", None),
        P(),
        P(None, "gz", "gy", None),
        P(None, "gz", "gy"),
    )
    return jax.shard_map(
        local,
        mesh=mesh,
        in_specs=placed,
        out_specs=P(None, ("parts", "gz"), "gy", None),
        check_vma=False,
    )
```

```python
import math

import jax
import jax.numpy as jnp
import numpy as np
from jax import lax
from jax.experimental import pallas as pl
from jax.experimental.pallas import tpu as pltpu
from jax.sharding import PartitionSpec as P

exchange_stiffness = 0.25
tensor_index = ((0, 3, 4), (3, 1, 5), (4, 5, 2))
highest = lax.Precision.HIGHEST
components = 12
swap = [(0, 1), (1, 0)]
bf16 = jnp.bfloat16
f32 = jnp.float32
limits = pltpu.CompilerParams(vmem_limit_bytes=20 * 2**20)


def wave(first, second, period):
    angle = 2.0 * np.pi / period * (np.outer(first, second) % period)
    return np.cos(angle), np.sin(angle)


def slot_frequencies(groups_z):
    bits = groups_z.bit_length() - 1
    reversed_bits = np.array([int(format(d, f"0{bits}b")[::-1], 2) for d in range(groups_z)])
    return np.concatenate([2 * reversed_bits, 2 * reversed_bits + 1])


def tables(columns, rows, groups_z):
    half = rows // 2
    x = np.arange(columns)
    y = np.arange(rows)
    ky = np.arange(2 * rows)
    z = np.arange(groups_z)
    out = {}
    cx, sx = wave(x, x, 2 * columns)
    out["tx"] = np.concatenate([cx, -sx], axis=1)
    forward, back = [], []
    for g in range(2):
        own_ky = ky[g * rows : (g + 1) * rows]
        there, here = [], []
        for h in (g, 1 - g):
            c, s = wave(y[h * half : (h + 1) * half], own_ky, 2 * rows)
            there.append(np.block([[c, -s], [s, c]]))
            here.append(np.block([[c.T, s.T], [-s.T, c.T]]))
        forward.append(np.concatenate(there, axis=0))
        back.append(np.concatenate(here, axis=1))
    out["ty"] = np.stack(forward)
    out["ty_back"] = np.stack(back)
    c, s = wave(slot_frequencies(groups_z), z, 2 * groups_z)
    out["tz"] = np.concatenate([c, s], axis=1)
    out["tz_back"] = np.concatenate([c.T, s.T], axis=1)
    w = np.where(x == 0, 1.0, 2.0)[:, None]
    scale = 1.0 / (2.0 * columns * 2.0 * rows * 2.0 * groups_z)
    out["tx_back"] = np.concatenate([w * cx, -w * sx], axis=1) * scale
    forward, back = [], []
    for g in range(2):
        c, s = wave(ky, y[g * half : (g + 1) * half], 2 * rows)
        c, s = c.reshape(2, rows, half), s.reshape(2, rows, half)
        forward.append(np.concatenate([c[0], -s[0], c[1], -s[1]], axis=1))
        back.append(np.stack([c[0], -s[0], c[1], -s[1]]) * scale)
    out["ny"] = np.stack(forward)
    out["ny_back"] = np.stack(back)
    return out


def halves(table):
    table = np.asarray(table, dtype=np.float32)
    high = table.astype(bf16)
    low = (table - high.astype(np.float32)).astype(bf16)
    return jnp.asarray(np.stack([high, low]))


def split(x):
    high = x.astype(bf16)
    return high, (x - high.astype(f32)).astype(bf16)


def three(left, right, dims=((1,), (0,))):
    (lh, ll), (rh, rl) = left, right
    prod = lambda a, b: lax.dot_general(a, b, (dims, ((), ())), preferred_element_type=f32)
    return prod(lh, rh) + (prod(lh, rl) + prod(ll, rh))


def cross(real, imag, lower):
    return jnp.concatenate([jnp.concatenate([real, imag], axis=1), lower], axis=0)


def prepare_kernel(share, mine_ref, sat_ref, dir_hbm, reg_hbm, main_hbm, nyq_hbm, tx_hbm, ny_hbm,
                   send_ref, stack_ref, dirs, reg, main, nyq, tx, ny, rows_t, sems):
    three_c, half, columns = dirs.shape
    width = 4 + share
    copies = [
        pltpu.make_async_copy(reg_hbm, reg, sems.at[0]),
        pltpu.make_async_copy(dir_hbm, dirs, sems.at[1]),
        pltpu.make_async_copy(main_hbm.at[pl.ds(mine_ref[0], share)], main, sems.at[2]),
        pltpu.make_async_copy(tx_hbm, tx, sems.at[3]),
        pltpu.make_async_copy(ny_hbm.at[mine_ref[1]], ny, sems.at[4]),
        pltpu.make_async_copy(nyq_hbm, nyq, sems.at[5]),
    ]
    for c in copies:
        c.start()
    rows_t[...] = jnp.zeros_like(rows_t)
    copies[0].wait()
    region = reg[...]
    magnetic = (region > 0).astype(f32)
    strength = jnp.zeros(region.shape, f32)
    for r in range(3):
        strength = strength + jnp.where(region == r + 1, sat_ref[r], 0.0)
    copies[1].wait()
    stack_ref[3] = magnetic
    lane = lax.broadcasted_iota(jnp.int32, (half, columns), 1)
    signs = (1 - 2 * (lane % 2)).astype(f32)
    moments = []
    sums = jnp.zeros((half, columns), f32)
    for c in range(3):
        one = dirs[c]
        stack_ref[c] = one * magnetic
        moment = one * strength
        moments.append(moment)
        total = jnp.sum(moment * signs, axis=1, keepdims=True)
        sums = jnp.where((lane % 4 == c) & (lane % 32 < 12), total, sums)
    copies[3].wait()
    zero = jnp.zeros((half, columns), bf16)
    table = (tx[0], tx[1])
    for c in range(3):
        high, low = split(moments[c])
        wide = [jnp.concatenate([jnp.concatenate([p, zero], 1), jnp.concatenate([zero, p], 1)], 0) for p in (high, low)]
        send_ref[pl.ds(c, columns, stride=width), :] = three(table, wide, ((1,), (1,)))
    copies[2].wait()
    for r in range(share):
        send_ref[pl.ds(4 + r, columns, stride=width), :] = main[r].T
    copies[4].wait()
    parts = [split(jnp.where(lane // 32 == q, sums, 0.0)) for q in range(4)]
    stacked = [jnp.concatenate([p[k] for p in parts], axis=0) for k in range(2)]
    row = three((ny[0], ny[1]), stacked)
    copies[5].wait()
    for s in range(2):
        for i in range(3):
            for j in range(3):
                rows_t[pl.ds(64 * s + 16 + 4 * i + j, 1), :] = nyq[tensor_index[i][j], pl.ds(s, 1), :]
    send_ref[pl.ds(3, columns, stride=width), :] = row + rows_t[...].T


def prepare(mine, saturation, direction, region, kernel_main, kernel_nyq, tx, ny, share):
    _, half, columns = direction.shape
    rows = kernel_main.shape[1]
    any_spec = pl.BlockSpec(memory_space=pltpu.HBM)
    smem = pl.BlockSpec(memory_space=pltpu.SMEM)
    vmem = pl.BlockSpec(memory_space=pltpu.VMEM)

    def body(*refs):
        prepare_kernel(share, *refs)

    return pl.pallas_call(
        body,
        name="prepare",
        compiler_params=limits,
        out_shape=(
            jax.ShapeDtypeStruct((columns * (4 + share), columns), f32),
            jax.ShapeDtypeStruct((4, half, columns), f32),
        ),
        in_specs=[smem, smem] + [any_spec] * 6,
        out_specs=(vmem, vmem),
        scratch_shapes=[
            pltpu.VMEM((3, half, columns), f32),
            pltpu.VMEM((half, columns), jnp.int32),
            pltpu.VMEM((share, rows, columns), f32),
            pltpu.VMEM(kernel_nyq.shape, f32),
            pltpu.VMEM(tx.shape, bf16),
            pltpu.VMEM(ny.shape[1:], bf16),
            pltpu.VMEM((columns, columns), f32),
            pltpu.SemaphoreType.DMA((6,)),
        ],
    )(mine, saturation, direction, region, kernel_main, kernel_nyq, tx, ny)


def forward_kernel(where_ref, own, other, ty, tz, out):
    planes, width = own.shape[1:]
    table = (tz[0], tz[1])
    y_table = (ty[0], ty[1])
    for c in range(4):
        if c < 3:
            ready = three(split(jnp.concatenate([own[c], other[c]], axis=1)), y_table)
            real, imag = ready[:, :width], ready[:, width:]
        else:
            lane = lax.broadcasted_iota(jnp.int32, (planes, width), 1)
            summed = own[3] + other[3]
            summed = jnp.where(where_ref[1] == 0, summed, pltpu.roll(summed, 64, 1))
            real = jnp.where(lane < 12, summed, 0.0)
            imag = jnp.where(lane < 12, pltpu.roll(summed, width - 32, 1), 0.0)
        (rh, rl), (ih, il) = split(real), split(imag)
        crossed = [cross(r, i, jnp.concatenate([i, -r], axis=1)) for r, i in ((rh, ih), (rl, il))]
        out[c] = three(table, crossed)


def forward(where, own, other, ty, tz):
    planes, width = own.shape[1:]
    smem = pl.BlockSpec(memory_space=pltpu.SMEM)
    vmem = pl.BlockSpec(memory_space=pltpu.VMEM)
    return pl.pallas_call(
        forward_kernel,
        name="forward",
        compiler_params=limits,
        out_shape=jax.ShapeDtypeStruct((4, 2 * planes, 2 * width), f32),
        in_specs=[smem] + [vmem] * 4,
        out_specs=vmem,
    )(where, own, other, ty, tz)


def inverse_kernel(parts, share, where_ref, *refs):
    spectra, row_ref, ty, tz, *shares, own, other = refs
    planes, width = row_ref.shape
    part = where_ref[2]
    table = (tz[0], tz[1])
    y_table = (ty[0], ty[1])

    def kernel_row(c):
        owner = c // share
        at = c - min(owner * share, components - share)
        piece = shares[0][at]
        for k in range(1, parts):
            gone = part - owner
            gone = jnp.where(gone < 0, gone + parts, gone)
            piece = jnp.where(gone == k, shares[k][at], piece)
        return piece

    def back(real, imag):
        (rh, rl), (ih, il) = split(real), split(imag)
        crossed = [cross(r, i, jnp.concatenate([-i, r], axis=1)) for r, i in ((rh, ih), (rl, il))]
        return three(table, crossed)

    kernel = [jnp.concatenate([kernel_row(2 * t), kernel_row(2 * t + 1)], axis=0) for t in range(6)]
    for i in range(3):
        real = imag = None
        for j in range(3):
            k = kernel[tensor_index[i][j]]
            a, b = k * spectra[j, :, :width], k * spectra[j, :, width:]
            real, imag = (a, b) if real is None else (real + a, imag + b)
        lines = three(split(back(real, imag)), y_table)
        own[pl.ds(i, planes, stride=4), :] = lines[:, :width]
        other[pl.ds(i, planes, stride=4), :] = lines[:, width:]
    lane = lax.broadcasted_iota(jnp.int32, (planes, width), 1)
    row = row_ref[...]
    k = jnp.concatenate([pltpu.roll(row, width - 16, 1), pltpu.roll(row, width - 80, 1)], axis=0)
    k = jnp.where(jnp.concatenate([lane, lane], axis=0) < 12, k, 0.0)
    line = back(spectra[3, :, :width] * k, spectra[3, :, width:] * k)
    line = line[:, :width] + pltpu.roll(line[:, width:], 32, 1)
    line = jnp.where(where_ref[1] == 0, line, pltpu.roll(line, 64, 1))
    own[pl.ds(3, planes, stride=4), :] = line
    other[pl.ds(3, planes, stride=4), :] = line


def inverse(where, spectra, row, ty, tz, shares, share):
    planes, width = row.shape
    smem = pl.BlockSpec(memory_space=pltpu.SMEM)
    vmem = pl.BlockSpec(memory_space=pltpu.VMEM)
    parts = len(shares)

    def body(*refs):
        inverse_kernel(parts, share, *refs)

    half = jax.ShapeDtypeStruct((4 * planes, width), f32)
    return pl.pallas_call(
        body,
        name="inverse",
        compiler_params=limits,
        out_shape=(half, half),
        in_specs=[smem] + [vmem] * (4 + parts),
        out_specs=(vmem, vmem),
    )(where, spectra, row, ty, tz, *shares)


def back_x(received, tx_back, ny_back, signs):
    columns = received.shape[0]
    half = received.shape[2] // 2
    main = received[:, :3].reshape(columns, 3, 2, half)
    table = tx_back.reshape(columns, 2, columns)
    demag = jnp.einsum("kcry,krx->cyx", main, table, precision=highest)
    extra = received[:, 3].reshape(columns, 4, 32)[:, :, :12].reshape(columns, 4, 3, 4)[..., :3].sum(axis=3)
    nyquist = jnp.einsum("gqi,qgy->iy", extra, ny_back, precision=highest)
    return demag + nyquist[:, :, None] * signs


def local(direction, region, saturation, kernel_main, kernel_nyq):
    columns = direction.shape[3]
    half = direction.shape[2]
    groups_z = lax.axis_size("gz")
    rows = half * lax.axis_size("gy")
    parts = lax.axis_size("parts")
    y_index = lax.axis_index("gy")
    part = lax.axis_index("parts")
    share = -(-components // parts)
    t = tables(columns, rows, groups_z)
    direction = direction[:, 0]
    where = jnp.stack([jnp.minimum(part * share, components - share), y_index, part])
    send, stacked = prepare(
        where, saturation, direction, region[0], kernel_main.reshape(components, rows, columns), kernel_nyq,
        halves(t["tx"]), halves(t["ny"]).swapaxes(0, 1), share,
    )
    width = 4 + share
    recv = lax.all_to_all(send.reshape(columns, width // 2, 2, columns), "gz", 0, 0, tiled=True)
    recv = recv.reshape(columns, width, columns).transpose(1, 0, 2)
    shares = [recv[4:]]
    for k in range(1, parts):
        shares.append(lax.ppermute(shares[0], "parts", [(p, (p + k) % parts) for p in range(parts)]))
    own_m = recv[:4]
    other_m = lax.ppermute(own_m, "gy", swap)
    up = [(i, i + 1) for i in range(groups_z - 1)]
    down = [(b, a) for a, b in up]
    stacked, other_m = lax.optimization_barrier((stacked, other_m))
    before = lax.ppermute(stacked, "gz", up)
    after = lax.ppermute(stacked, "gz", down)
    edge = jnp.where(y_index == 0, stacked[:, -1], stacked[:, 0])
    edge = lax.ppermute(edge, "gy", swap)
    ty = halves(t["ty"])[:, y_index]
    ty_back = halves(t["ty_back"])[:, y_index]
    spectra = forward(where, own_m, other_m, ty, halves(t["tz"]))
    own, other = inverse(where, spectra, own_m[3], ty_back, halves(t["tz_back"]), shares, share)
    own, other = (a.reshape(groups_z, 4, columns) for a in (own, other))
    other, before, after, edge = lax.optimization_barrier((other, before, after, edge))
    send_f = own + lax.ppermute(other, "gy", swap)
    recv_f = lax.all_to_all(send_f, "gz", 0, 0, tiled=True)
    magnetic = stacked[3:4]
    low = jnp.where(y_index == 0, 0.0, edge)[:, None]
    high = jnp.where(y_index == 0, edge, 0.0)[:, None]
    tall = jnp.concatenate([low, stacked, high], axis=1)
    wide = jnp.pad(stacked, ((0, 0), (0, 0), (1, 1)))
    near = before + after + tall[:, :-2] + tall[:, 2:] + wide[..., :-2] + wide[..., 2:]
    exchange = exchange_stiffness * magnetic * (near[:3] - near[3:4] * direction)
    signs = (1.0 - 2.0 * (jnp.arange(columns) % 2)).astype(f32)
    demag = back_x(recv_f, jnp.asarray(t["tx_back"], f32), jnp.asarray(t["ny_back"], f32)[y_index], signs)
    return (demag + exchange)[:, None]


def solution(mesh):
    placed = (
        P(None, ("parts", "gz"), "gy", None),
        P(("parts", "gz"), "gy", None),
        P(),
        P(None, "gz", "gy", None),
        P(None, "gz", "gy"),
    )
    return jax.shard_map(
        local,
        mesh=mesh,
        in_specs=placed,
        out_specs=P(None, ("parts", "gz"), "gy", None),
        check_vma=False,
    )
```

```python
import jax
import jax.numpy as jnp
import numpy as np
from jax import lax
from jax.experimental import pallas as pl
from jax.experimental.pallas import tpu as pltpu
from jax.sharding import PartitionSpec as P


exchange_stiffness = 0.25
tensor_index = ((0, 3, 4), (3, 1, 5), (4, 5, 2))
components = 12
swap = [(0, 1), (1, 0)]
bf16 = jnp.bfloat16
f32 = jnp.float32
limits = pltpu.CompilerParams(vmem_limit_bytes=20 * 2**20)


def wave(first, second, period):
    angle = 2.0 * np.pi / period * (np.outer(first, second) % period)
    return np.cos(angle), np.sin(angle)


def slot_frequencies(groups_z):
    bits = groups_z.bit_length() - 1
    reversed_bits = np.array([int(format(d, f"0{bits}b")[::-1], 2) for d in range(groups_z)])
    return np.concatenate([2 * reversed_bits, 2 * reversed_bits + 1])


def tables(columns, rows, groups_z):
    half = rows // 2
    x = np.arange(columns)
    y = np.arange(rows)
    ky = np.arange(2 * rows)
    z = np.arange(groups_z)
    out = {}
    cx, sx = wave(x, x, 2 * columns)
    out["tx"] = np.concatenate([cx, -sx], axis=1)
    forward, back = [], []
    for g in range(2):
        own_ky = ky[g * rows : (g + 1) * rows]
        there, here = [], []
        for h in (g, 1 - g):
            c, s = wave(y[h * half : (h + 1) * half], own_ky, 2 * rows)
            there.append(np.block([[c, -s], [s, c]]))
            here.append(np.block([[c.T, s.T], [-s.T, c.T]]))
        forward.append(np.concatenate(there, axis=0))
        back.append(np.concatenate(here, axis=1))
    out["ty"] = np.stack(forward)
    out["ty_back"] = np.stack(back)
    c, s = wave(slot_frequencies(groups_z), z, 2 * groups_z)
    out["tz"] = np.concatenate([c, s], axis=1)
    out["tz_back"] = np.concatenate([c.T, s.T], axis=1)
    w = np.where(x == 0, 1.0, 2.0)[:, None]
    scale = 1.0 / (2.0 * columns * 2.0 * rows * 2.0 * groups_z)
    out["tx_back"] = np.concatenate([w * cx, -w * sx], axis=1) * scale
    forward, back = [], []
    for g in range(2):
        c, s = wave(ky, y[g * half : (g + 1) * half], 2 * rows)
        c, s = c.reshape(2, rows, half), s.reshape(2, rows, half)
        forward.append(np.concatenate([c[0], -s[0], c[1], -s[1]], axis=1))
        back.append(np.concatenate([c[0].T, -s[0].T, c[1].T, -s[1].T], axis=0) * scale)
    out["ny"] = np.stack(forward)
    out["ny_back"] = np.stack(back)
    return out


def halves(table):
    table = np.asarray(table, dtype=np.float32)
    high = table.astype(bf16)
    low = (table - high.astype(np.float32)).astype(bf16)
    return jnp.asarray(np.stack([high, low]))


def split(x):
    high = x.astype(bf16)
    return high, (x - high.astype(f32)).astype(bf16)


def three(left, right, dims=((1,), (0,))):
    (lh, ll), (rh, rl) = left, right
    prod = lambda a, b: lax.dot_general(a, b, (dims, ((), ())), preferred_element_type=f32)
    return prod(lh, rh) + (prod(lh, rl) + prod(ll, rh))


def cross(real, imag, lower):
    return jnp.concatenate([jnp.concatenate([real, imag], axis=1), lower], axis=0)


def prepare_kernel(share, mine_ref, sat_ref, dir_hbm, reg_hbm, main_hbm, nyq_hbm, tx_hbm, ny_hbm,
                   send_ref, stack_ref, dirs, reg, main, nyq, tx, ny, rows_t, sems):
    _, half, columns = dirs.shape
    width = 4 + share
    copies = [
        pltpu.make_async_copy(reg_hbm, reg, sems.at[0]),
        pltpu.make_async_copy(dir_hbm, dirs, sems.at[1]),
        pltpu.make_async_copy(main_hbm.at[pl.ds(mine_ref[0], share)], main, sems.at[2]),
        pltpu.make_async_copy(tx_hbm, tx, sems.at[3]),
        pltpu.make_async_copy(ny_hbm.at[mine_ref[1]], ny, sems.at[4]),
        pltpu.make_async_copy(nyq_hbm, nyq, sems.at[5]),
    ]
    for c in copies:
        c.start()
    rows_t[...] = jnp.zeros_like(rows_t)
    copies[0].wait()
    region = reg[...]
    magnetic = (region > 0).astype(f32)
    strength = jnp.zeros(region.shape, f32)
    for r in range(3):
        strength = strength + jnp.where(region == r + 1, sat_ref[r], 0.0)
    copies[1].wait()
    stack_ref[3] = magnetic
    lane = lax.broadcasted_iota(jnp.int32, (half, columns), 1)
    signs = (1 - 2 * (lane % 2)).astype(f32)
    moments = []
    sums = jnp.zeros((half, columns), f32)
    for c in range(3):
        one = dirs[c]
        stack_ref[c] = one * magnetic
        moment = one * strength
        moments.append(moment)
        total = jnp.sum(moment * signs, axis=1, keepdims=True)
        sums = jnp.where((lane % 4 == c) & (lane % 32 < 12), total, sums)
    copies[3].wait()
    zero = jnp.zeros((half, columns), bf16)
    table = (tx[0], tx[1])
    for c in range(3):
        high, low = split(moments[c])
        wide = [jnp.concatenate([jnp.concatenate([p, zero], 1), jnp.concatenate([zero, p], 1)], 0) for p in (high, low)]
        send_ref[pl.ds(c, columns, stride=width), :] = three(table, wide, ((1,), (1,)))
    copies[2].wait()
    for r in range(share):
        send_ref[pl.ds(4 + r, columns, stride=width), :] = main[r].T
    copies[4].wait()
    parts = [split(jnp.where(lane // 32 == q, sums, 0.0)) for q in range(4)]
    stacked = [jnp.concatenate([p[k] for p in parts], axis=0) for k in range(2)]
    row = three((ny[0], ny[1]), stacked)
    copies[5].wait()
    for s in range(2):
        for i in range(3):
            for j in range(3):
                rows_t[pl.ds(64 * s + 16 + 4 * i + j, 1), :] = nyq[tensor_index[i][j], pl.ds(s, 1), :]
    send_ref[pl.ds(3, columns, stride=width), :] = row + rows_t[...].T


def prepare(mine, saturation, direction, region, kernel_main, kernel_nyq, tx, ny, share):
    _, half, columns = direction.shape
    rows = kernel_main.shape[1]
    any_spec = pl.BlockSpec(memory_space=pltpu.HBM)
    smem = pl.BlockSpec(memory_space=pltpu.SMEM)
    vmem = pl.BlockSpec(memory_space=pltpu.VMEM)

    def body(*refs):
        prepare_kernel(share, *refs)

    return pl.pallas_call(
        body,
        name="prepare",
        compiler_params=limits,
        out_shape=(
            jax.ShapeDtypeStruct((columns * (4 + share), columns), f32),
            jax.ShapeDtypeStruct((4, half, columns), f32),
        ),
        in_specs=[smem, smem] + [any_spec] * 6,
        out_specs=(vmem, vmem),
        scratch_shapes=[
            pltpu.VMEM((3, half, columns), f32),
            pltpu.VMEM((half, columns), jnp.int32),
            pltpu.VMEM((share, rows, columns), f32),
            pltpu.VMEM(kernel_nyq.shape, f32),
            pltpu.VMEM(tx.shape, bf16),
            pltpu.VMEM(ny.shape[1:], bf16),
            pltpu.VMEM((columns, columns), f32),
            pltpu.SemaphoreType.DMA((6,)),
        ],
    )(mine, saturation, *(pltpu.with_memory_space_constraint(a, pltpu.HBM) for a in (direction, region, kernel_main, kernel_nyq, tx, ny)))


def forward_kernel(where_ref, own, other, ty, tz, out):
    planes, width = own.shape[1:]
    table = (tz[0], tz[1])
    y_table = (ty[0, where_ref[1]], ty[1, where_ref[1]])
    for c in range(4):
        if c < 3:
            ready = three(split(jnp.concatenate([own[c], other[c]], axis=1)), y_table)
            real, imag = ready[:, :width], ready[:, width:]
        else:
            lane = lax.broadcasted_iota(jnp.int32, (planes, width), 1)
            summed = own[3] + other[3]
            summed = jnp.where(where_ref[1] == 0, summed, pltpu.roll(summed, 64, 1))
            real = jnp.where(lane < 12, summed, 0.0)
            imag = jnp.where(lane < 12, pltpu.roll(summed, width - 32, 1), 0.0)
        (rh, rl), (ih, il) = split(real), split(imag)
        crossed = [cross(r, i, jnp.concatenate([i, -r], axis=1)) for r, i in ((rh, ih), (rl, il))]
        out[c] = three(table, crossed)


def forward(where, own, other, ty, tz):
    planes, width = own.shape[1:]
    smem = pl.BlockSpec(memory_space=pltpu.SMEM)
    vmem = pl.BlockSpec(memory_space=pltpu.VMEM)
    return pl.pallas_call(
        forward_kernel,
        name="forward",
        compiler_params=limits,
        out_shape=jax.ShapeDtypeStruct((4, 2 * planes, 2 * width), f32),
        in_specs=[smem] + [vmem] * 4,
        out_specs=vmem,
    )(where, own, other, ty, tz)


def inverse_kernel(parts, share, where_ref, *refs):
    spectra, row_ref, stack, ty, tz, *shares, own, other = refs
    planes, width = row_ref.shape
    part = where_ref[2]
    table = (tz[0], tz[1])
    y_table = (ty[0, where_ref[1]], ty[1, where_ref[1]])

    def kernel_row(c):
        owner = c // share
        at = c - min(owner * share, components - share)
        piece = shares[0][at]
        for k in range(1, parts):
            gone = part - owner
            gone = jnp.where(gone < 0, gone + parts, gone)
            piece = jnp.where(gone == k, shares[k][at], piece)
        return piece

    def back(real, imag):
        (rh, rl), (ih, il) = split(real), split(imag)
        crossed = [cross(r, i, jnp.concatenate([-i, r], axis=1)) for r, i in ((rh, ih), (rl, il))]
        return three(table, crossed)

    kernel = [jnp.concatenate([kernel_row(2 * t), kernel_row(2 * t + 1)], axis=0) for t in range(6)]
    for i in range(3):
        real = imag = None
        for j in range(3):
            k = kernel[tensor_index[i][j]]
            a, b = k * spectra[j, :, :width], k * spectra[j, :, width:]
            real, imag = (a, b) if real is None else (real + a, imag + b)
        lines = three(split(back(real, imag)), y_table)
        own[pl.ds(i, planes, stride=4), :] = lines[:, :width]
        other[pl.ds(i, planes, stride=4), :] = lines[:, width:]
    lane = lax.broadcasted_iota(jnp.int32, (planes, width), 1)
    row = row_ref[...]
    k = jnp.concatenate([pltpu.roll(row, width - 16, 1), pltpu.roll(row, width - 80, 1)], axis=0)
    k = jnp.where(jnp.concatenate([lane, lane], axis=0) < 12, k, 0.0)
    line = back(spectra[3, :, :width] * k, spectra[3, :, width:] * k)
    line = line[:, :width] + pltpu.roll(line[:, width:], 32, 1)
    line = jnp.where(where_ref[1] == 0, line, pltpu.roll(line, 64, 1))
    own[pl.ds(3, planes, stride=4), :] = line
    other[pl.ds(3, planes, stride=4), :] = line
    last = stack.shape[1] - 1
    for c in range(4):
        edge = jnp.where(where_ref[1] == 0, stack[c, last:], stack[c, :1])
        other[4 * planes + c : 4 * planes + c + 1, :] = edge
        other[4 * planes + 4 + c : 4 * planes + 5 + c, :] = edge


def inverse(where, spectra, row, stacked, ty, tz, shares, share):
    planes, width = row.shape
    smem = pl.BlockSpec(memory_space=pltpu.SMEM)
    vmem = pl.BlockSpec(memory_space=pltpu.VMEM)
    parts = len(shares)

    def body(*refs):
        inverse_kernel(parts, share, *refs)

    shape = lambda rows: jax.ShapeDtypeStruct((rows, width), f32)
    return pl.pallas_call(
        body,
        name="inverse",
        compiler_params=limits,
        out_shape=(shape(4 * planes), shape(4 * planes + 8)),
        in_specs=[smem] + [vmem] * (5 + parts),
        out_specs=(vmem, vmem),
    )(where, spectra, row, stacked, ty, tz, *shares)


def finish_kernel(where_ref, recv, arrived, stack, before, after, tx, ny, out):
    _, half, columns = stack.shape
    lane = lax.broadcasted_iota(jnp.int32, (half, columns), 1)
    line = lax.broadcasted_iota(jnp.int32, (half, columns), 0)
    signs = (1 - 2 * (lane % 2)).astype(f32)
    lower = where_ref[1] == 0

    def near(c):
        one = stack[c]
        edge = arrived[pl.ds(4 * columns + c, 1), :]
        low = jnp.where(line == 0, jnp.where(lower, 0.0, edge), pltpu.roll(one, 1, 0))
        high = jnp.where(line == half - 1, jnp.where(lower, edge, 0.0), pltpu.roll(one, half - 1, 0))
        left = jnp.where(lane == 0, 0.0, pltpu.roll(one, 1, 1))
        right = jnp.where(lane == columns - 1, 0.0, pltpu.roll(one, columns - 1, 1))
        return before[c] + after[c] + low + high + left + right

    count = near(3)
    magnetic = stack[3]
    nyquist = three((ny[0, where_ref[1]], ny[1, where_ref[1]]), split(recv[pl.ds(3, columns, stride=4), :]))
    sums = jnp.zeros((half, columns), f32)
    for q in range(4):
        sums = jnp.where(lane // 32 == q, nyquist[q * half : (q + 1) * half], sums)
    table = (tx[0], tx[1])
    for c in range(3):
        prod = three(split(recv[pl.ds(c, columns, stride=4), :].T), table)
        demag = prod[:half, :columns] + prod[half:, columns:]
        total = jnp.sum(jnp.where(lane % 32 // 4 == c, sums, 0.0), axis=1, keepdims=True)
        exchange = exchange_stiffness * (magnetic * near(c) - count * stack[c])
        out[c] = demag + total * signs + exchange


def finish(where, recv, arrived, stacked, before, after, tx, ny):
    smem = pl.BlockSpec(memory_space=pltpu.SMEM)
    vmem = pl.BlockSpec(memory_space=pltpu.VMEM)
    return pl.pallas_call(
        finish_kernel,
        name="finish",
        compiler_params=limits,
        out_shape=jax.ShapeDtypeStruct((3,) + stacked.shape[1:], f32),
        in_specs=[smem] + [vmem] * 7,
        out_specs=vmem,
    )(where, recv, arrived, stacked, before, after, tx, ny)


def local(direction, region, saturation, kernel_main, kernel_nyq):
    columns = direction.shape[3]
    half = direction.shape[2]
    groups_z = lax.axis_size("gz")
    rows = half * lax.axis_size("gy")
    parts = lax.axis_size("parts")
    y_index = lax.axis_index("gy")
    part = lax.axis_index("parts")
    share = -(-components // parts)
    t = tables(columns, rows, groups_z)
    direction = direction[:, 0]
    where = jnp.stack([jnp.minimum(part * share, components - share), y_index, part])
    send, stacked = prepare(
        where, saturation, direction, region[0], kernel_main.reshape(components, rows, columns), kernel_nyq,
        halves(t["tx"]), halves(t["ny"]).swapaxes(0, 1), share,
    )
    width = 4 + share
    recv = lax.all_to_all(send.reshape(columns, width // 2, 2, columns), "gz", 0, 0, tiled=True)
    recv = recv.reshape(columns, width, columns).transpose(1, 0, 2)
    shares = [recv[4:]]
    for k in range(1, parts):
        shares.append(lax.ppermute(shares[0], "parts", [(p, (p + k) % parts) for p in range(parts)]))
    own_m = recv[:4]
    other_m = lax.ppermute(own_m, "gy", swap)
    up = [(i, i + 1) for i in range(groups_z - 1)]
    down = [(b, a) for a, b in up]
    stacked, other_m = lax.optimization_barrier((stacked, other_m))
    before = lax.ppermute(stacked, "gz", up)
    after = lax.ppermute(stacked, "gz", down)
    spectra = forward(where, own_m, other_m, halves(t["ty"]), halves(t["tz"]))
    own, other = inverse(where, spectra, own_m[3], stacked, halves(t["ty_back"]), halves(t["tz_back"]), shares, share)
    other, before, after = lax.optimization_barrier((other, before, after))
    arrived = lax.ppermute(other, "gy", swap)
    send_f = own + arrived[: 4 * groups_z]
    recv_f = lax.all_to_all(send_f.reshape(groups_z, 4, columns), "gz", 0, 0, tiled=True)
    recv_f = recv_f.reshape(4 * columns, columns)
    tx_back, ny_back = halves(t["tx_back"]), halves(t["ny_back"])
    return finish(where, recv_f, arrived, stacked, before, after, tx_back, ny_back)[:, None]


def solution(mesh):
    placed = (
        P(None, ("parts", "gz"), "gy", None),
        P(("parts", "gz"), "gy", None),
        P(),
        P(None, "gz", "gy", None),
        P(None, "gz", "gy"),
    )

    return jax.shard_map(
        local,
        mesh=mesh,
        in_specs=placed,
        out_specs=P(None, ("parts", "gz"), "gy", None),
        check_vma=False,
    )
```

```python
import jax
import jax.numpy as jnp
import numpy as np
from jax import lax
from jax.experimental import pallas as pl
from jax.experimental.pallas import tpu as pltpu
from jax.sharding import PartitionSpec as P


exchange_stiffness = 0.25
tensor_index = ((0, 3, 4), (3, 1, 5), (4, 5, 2))
components = 12
swap = [(0, 1), (1, 0)]
bf16 = jnp.bfloat16
f32 = jnp.float32
limits = pltpu.CompilerParams(vmem_limit_bytes=20 * 2**20)


def wave(first, second, period):
    angle = 2.0 * np.pi / period * (np.outer(first, second) % period)
    return np.cos(angle), np.sin(angle)


def slot_frequencies(groups_z):
    bits = groups_z.bit_length() - 1
    reversed_bits = np.array([int(format(d, f"0{bits}b")[::-1], 2) for d in range(groups_z)])
    return np.concatenate([2 * reversed_bits, 2 * reversed_bits + 1])


def tables(columns, rows, groups_z):
    half = rows // 2
    x = np.arange(columns)
    y = np.arange(rows)
    ky = np.arange(2 * rows)
    z = np.arange(groups_z)
    out = {}
    cx, sx = wave(x, x, 2 * columns)
    out["tx"] = np.concatenate([cx, -sx], axis=1)
    forward, back = [], []
    for g in range(2):
        own_ky = ky[g * rows : (g + 1) * rows]
        there, here = [], []
        for h in (g, 1 - g):
            c, s = wave(y[h * half : (h + 1) * half], own_ky, 2 * rows)
            there.append(np.block([[c, -s], [s, c]]))
            here.append(np.block([[c.T, s.T], [-s.T, c.T]]))
        forward.append(np.concatenate(there, axis=0))
        back.append(np.concatenate(here, axis=1))
    out["ty"] = np.stack(forward)
    out["ty_back"] = np.stack(back)
    c, s = wave(slot_frequencies(groups_z), z, 2 * groups_z)
    out["tz"] = np.concatenate([c, s], axis=1)
    out["tz_back"] = np.concatenate([c.T, s.T], axis=1)
    w = np.where(x == 0, 1.0, 2.0)[:, None]
    scale = 1.0 / (2.0 * columns * 2.0 * rows * 2.0 * groups_z)
    out["tx_back"] = np.concatenate([w * cx, -w * sx], axis=1) * scale
    forward, back = [], []
    for g in range(2):
        c, s = wave(ky, y[g * half : (g + 1) * half], 2 * rows)
        c, s = c.reshape(2, rows, half), s.reshape(2, rows, half)
        forward.append(np.concatenate([c[0], -s[0], c[1], -s[1]], axis=1))
        back.append(np.concatenate([c[0].T, -s[0].T, c[1].T, -s[1].T], axis=0) * scale)
    out["ny"] = np.stack(forward)
    out["ny_back"] = np.stack(back)
    return out


def halves(table):
    table = np.asarray(table, dtype=np.float32)
    high = table.astype(bf16)
    low = (table - high.astype(np.float32)).astype(bf16)
    return jnp.asarray(np.stack([high, low]))


def split(x):
    high = x.astype(bf16)
    return high, (x - high.astype(f32)).astype(bf16)


def three(left, right, dims=((1,), (0,))):
    (lh, ll), (rh, rl) = left, right
    prod = lambda a, b: lax.dot_general(a, b, (dims, ((), ())), preferred_element_type=f32)
    return prod(lh, rh) + (prod(lh, rl) + prod(ll, rh))


def cross(real, imag, lower):
    return jnp.concatenate([jnp.concatenate([real, imag], axis=1), lower], axis=0)


def prepare_kernel(share, mine_ref, sat_hbm, dir_hbm, reg_hbm, main_hbm, nyq_hbm, tx_hbm, ny_hbm,
                   send_ref, stack_ref, sat_ref, dirs, reg, main, nyq, tx, ny, rows_t, sems):
    _, half, columns = dirs.shape
    width = 4 + share
    copies = [
        pltpu.make_async_copy(reg_hbm, reg, sems.at[0]),
        pltpu.make_async_copy(dir_hbm, dirs, sems.at[1]),
        pltpu.make_async_copy(main_hbm.at[pl.ds(mine_ref[0], share)], main, sems.at[2]),
        pltpu.make_async_copy(tx_hbm, tx, sems.at[3]),
        pltpu.make_async_copy(ny_hbm.at[mine_ref[1]], ny, sems.at[4]),
        pltpu.make_async_copy(nyq_hbm, nyq, sems.at[5]),
        pltpu.make_async_copy(sat_hbm, sat_ref, sems.at[6]),
    ]
    for c in copies:
        c.start()
    rows_t[...] = jnp.zeros_like(rows_t)
    copies[0].wait()
    region = reg[...]
    magnetic = (region > 0).astype(f32)
    strength = jnp.zeros(region.shape, f32)
    copies[6].wait()
    for r in range(3):
        strength = strength + jnp.where(region == r + 1, sat_ref[r], 0.0)
    copies[1].wait()
    stack_ref[3] = magnetic
    lane = lax.broadcasted_iota(jnp.int32, (half, columns), 1)
    signs = (1 - 2 * (lane % 2)).astype(f32)
    moments = []
    sums = jnp.zeros((half, columns), f32)
    for c in range(3):
        one = dirs[c]
        stack_ref[c] = one * magnetic
        moment = one * strength
        moments.append(moment)
        total = jnp.sum(moment * signs, axis=1, keepdims=True)
        sums = jnp.where((lane % 4 == c) & (lane % 32 < 12), total, sums)
    copies[3].wait()
    zero = jnp.zeros((half, columns), bf16)
    table = (tx[0], tx[1])
    for c in range(3):
        high, low = split(moments[c])
        wide = [jnp.concatenate([jnp.concatenate([p, zero], 1), jnp.concatenate([zero, p], 1)], 0) for p in (high, low)]
        send_ref[pl.ds(c, columns, stride=width), :] = three(table, wide, ((1,), (1,)))
    copies[2].wait()
    for r in range(share):
        send_ref[pl.ds(4 + r, columns, stride=width), :] = main[r].T
    copies[4].wait()
    parts = [split(jnp.where(lane // 32 == q, sums, 0.0)) for q in range(4)]
    stacked = [jnp.concatenate([p[k] for p in parts], axis=0) for k in range(2)]
    row = three((ny[0], ny[1]), stacked)
    copies[5].wait()
    for s in range(2):
        for i in range(3):
            for j in range(3):
                rows_t[pl.ds(64 * s + 16 + 4 * i + j, 1), :] = nyq[tensor_index[i][j], pl.ds(s, 1), :]
    send_ref[pl.ds(3, columns, stride=width), :] = row + rows_t[...].T


def prepare(mine, saturation, direction, region, kernel_main, kernel_nyq, tx, ny, share):
    _, half, columns = direction.shape
    rows = kernel_main.shape[1]
    any_spec = pl.BlockSpec(memory_space=pltpu.HBM)
    smem = pl.BlockSpec(memory_space=pltpu.SMEM)
    vmem = pl.BlockSpec(memory_space=pltpu.VMEM)

    def body(*refs):
        prepare_kernel(share, *refs)

    return pl.pallas_call(
        body,
        name="prepare",
        compiler_params=limits,
        out_shape=(
            jax.ShapeDtypeStruct((columns * (4 + share), columns), f32),
            jax.ShapeDtypeStruct((4, half, columns), f32),
        ),
        in_specs=[smem] + [any_spec] * 7,
        out_specs=(vmem, vmem),
        scratch_shapes=[
            pltpu.SMEM(saturation.shape, f32),
            pltpu.VMEM((3, half, columns), f32),
            pltpu.VMEM((half, columns), jnp.int32),
            pltpu.VMEM((share, rows, columns), f32),
            pltpu.VMEM(kernel_nyq.shape, f32),
            pltpu.VMEM(tx.shape, bf16),
            pltpu.VMEM(ny.shape[1:], bf16),
            pltpu.VMEM((columns, columns), f32),
            pltpu.SemaphoreType.DMA((7,)),
        ],
    )(mine, *(pltpu.with_memory_space_constraint(a, pltpu.HBM) for a in (saturation, direction, region, kernel_main, kernel_nyq, tx, ny)))


def forward_kernel(where_ref, own, other, ty, tz, out):
    planes, width = own.shape[1:]
    table = (tz[0], tz[1])
    y_table = (ty[0, where_ref[1]], ty[1, where_ref[1]])
    for c in range(4):
        if c < 3:
            ready = three(split(jnp.concatenate([own[c], other[c]], axis=1)), y_table)
            real, imag = ready[:, :width], ready[:, width:]
        else:
            lane = lax.broadcasted_iota(jnp.int32, (planes, width), 1)
            summed = own[3] + other[3]
            summed = jnp.where(where_ref[1] == 0, summed, pltpu.roll(summed, 64, 1))
            real = jnp.where(lane < 12, summed, 0.0)
            imag = jnp.where(lane < 12, pltpu.roll(summed, width - 32, 1), 0.0)
        (rh, rl), (ih, il) = split(real), split(imag)
        crossed = [cross(r, i, jnp.concatenate([i, -r], axis=1)) for r, i in ((rh, ih), (rl, il))]
        out[c] = three(table, crossed)


def forward(where, own, other, ty, tz):
    planes, width = own.shape[1:]
    smem = pl.BlockSpec(memory_space=pltpu.SMEM)
    vmem = pl.BlockSpec(memory_space=pltpu.VMEM)
    return pl.pallas_call(
        forward_kernel,
        name="forward",
        compiler_params=limits,
        out_shape=jax.ShapeDtypeStruct((4, 2 * planes, 2 * width), f32),
        in_specs=[smem] + [vmem] * 4,
        out_specs=vmem,
    )(where, own, other, ty, tz)


def inverse_kernel(pairs, share, where_ref, *refs):
    spectra, row_ref, stack, ty, tz, *shares, own, other = refs
    planes, width = row_ref.shape
    table = (tz[0], tz[1])
    y_table = (ty[0, where_ref[1]], ty[1, where_ref[1]])

    def kernel_row(c):
        owner, at = c // share, c % share
        if pairs == 1:
            return shares[0][at]
        return jnp.where(where_ref[2] == owner, shares[0][at], shares[1][at])

    def back(real, imag):
        (rh, rl), (ih, il) = split(real), split(imag)
        crossed = [cross(r, i, jnp.concatenate([-i, r], axis=1)) for r, i in ((rh, ih), (rl, il))]
        return three(table, crossed)

    kernel = [jnp.concatenate([kernel_row(2 * t), kernel_row(2 * t + 1)], axis=0) for t in range(6)]
    for i in range(3):
        real = imag = None
        for j in range(3):
            k = kernel[tensor_index[i][j]]
            a, b = k * spectra[j, :, :width], k * spectra[j, :, width:]
            real, imag = (a, b) if real is None else (real + a, imag + b)
        lines = three(split(back(real, imag)), y_table)
        own[pl.ds(i, planes, stride=4), :] = lines[:, :width]
        other[pl.ds(i, planes, stride=4), :] = lines[:, width:]
    lane = lax.broadcasted_iota(jnp.int32, (planes, width), 1)
    row = row_ref[...]
    k = jnp.concatenate([pltpu.roll(row, width - 16, 1), pltpu.roll(row, width - 80, 1)], axis=0)
    k = jnp.where(jnp.concatenate([lane, lane], axis=0) < 12, k, 0.0)
    line = back(spectra[3, :, :width] * k, spectra[3, :, width:] * k)
    line = line[:, :width] + pltpu.roll(line[:, width:], 32, 1)
    line = jnp.where(where_ref[1] == 0, line, pltpu.roll(line, 64, 1))
    own[pl.ds(3, planes, stride=4), :] = line
    other[pl.ds(3, planes, stride=4), :] = line
    last = stack.shape[1] - 1
    for c in range(4):
        edge = jnp.where(where_ref[1] == 0, stack[c, last:], stack[c, :1])
        other[4 * planes + c : 4 * planes + c + 1, :] = edge
        other[4 * planes + 4 + c : 4 * planes + 5 + c, :] = edge


def inverse(where, spectra, row, stacked, ty, tz, shares, share):
    planes, width = row.shape
    smem = pl.BlockSpec(memory_space=pltpu.SMEM)
    vmem = pl.BlockSpec(memory_space=pltpu.VMEM)
    pairs = len(shares)

    def body(*refs):
        inverse_kernel(pairs, share, *refs)

    shape = lambda rows: jax.ShapeDtypeStruct((rows, width), f32)
    return pl.pallas_call(
        body,
        name="inverse",
        compiler_params=limits,
        out_shape=(shape(4 * planes), shape(4 * planes + 8)),
        in_specs=[smem] + [vmem] * (5 + pairs),
        out_specs=(vmem, vmem),
    )(where, spectra, row, stacked, ty, tz, *shares)


def finish_kernel(where_ref, recv, arrived, stack, before, after, tx, ny, out):
    _, half, columns = stack.shape
    lane = lax.broadcasted_iota(jnp.int32, (half, columns), 1)
    line = lax.broadcasted_iota(jnp.int32, (half, columns), 0)
    signs = (1 - 2 * (lane % 2)).astype(f32)
    lower = where_ref[1] == 0

    def near(c):
        one = stack[c]
        edge = arrived[pl.ds(4 * columns + c, 1), :]
        low = jnp.where(line == 0, jnp.where(lower, 0.0, edge), pltpu.roll(one, 1, 0))
        high = jnp.where(line == half - 1, jnp.where(lower, edge, 0.0), pltpu.roll(one, half - 1, 0))
        left = jnp.where(lane == 0, 0.0, pltpu.roll(one, 1, 1))
        right = jnp.where(lane == columns - 1, 0.0, pltpu.roll(one, columns - 1, 1))
        return before[c] + after[c] + low + high + left + right

    count = near(3)
    magnetic = stack[3]
    nyquist = three((ny[0, where_ref[1]], ny[1, where_ref[1]]), split(recv[pl.ds(3, columns, stride=4), :]))
    sums = jnp.zeros((half, columns), f32)
    for q in range(4):
        sums = jnp.where(lane // 32 == q, nyquist[q * half : (q + 1) * half], sums)
    table = (tx[0], tx[1])
    for c in range(3):
        prod = three(split(recv[pl.ds(c, columns, stride=4), :].T), table)
        demag = prod[:half, :columns] + prod[half:, columns:]
        total = jnp.sum(jnp.where(lane % 32 // 4 == c, sums, 0.0), axis=1, keepdims=True)
        exchange = exchange_stiffness * (magnetic * near(c) - count * stack[c])
        out[c] = demag + total * signs + exchange


def finish(where, recv, arrived, stacked, before, after, tx, ny):
    smem = pl.BlockSpec(memory_space=pltpu.SMEM)
    vmem = pl.BlockSpec(memory_space=pltpu.VMEM)
    return pl.pallas_call(
        finish_kernel,
        name="finish",
        compiler_params=limits,
        out_shape=jax.ShapeDtypeStruct((3,) + stacked.shape[1:], f32),
        in_specs=[smem] + [vmem] * 7,
        out_specs=vmem,
    )(where, recv, arrived, stacked, before, after, tx, ny)


def local(direction, region, saturation, kernel_main, kernel_nyq):
    columns = direction.shape[3]
    half = direction.shape[2]
    groups_z = lax.axis_size("gz")
    rows = half * lax.axis_size("gy")
    parts = lax.axis_size("parts")
    y_index = lax.axis_index("gy")
    part = lax.axis_index("parts")
    pairs = 2 if parts % 2 == 0 else 1
    share = components // pairs
    t = tables(columns, rows, groups_z)
    direction = direction[:, 0]
    where = jnp.stack([part % pairs * share, y_index, part % pairs])
    send, stacked = prepare(
        where, saturation, direction, region[0], kernel_main.reshape(components, rows, columns), kernel_nyq,
        halves(t["tx"]), halves(t["ny"]).swapaxes(0, 1), share,
    )
    width = 4 + share
    recv = lax.all_to_all(send.reshape(columns, width // 2, 2, columns), "gz", 0, 0, tiled=True)
    recv = recv.reshape(columns, width, columns).transpose(1, 0, 2)
    shares = [recv[4:]]
    if pairs == 2:
        shares.append(lax.ppermute(shares[0], "parts", [(p, p ^ 1) for p in range(parts)]))
    own_m = recv[:4]
    other_m = lax.ppermute(own_m, "gy", swap)
    up = [(i, i + 1) for i in range(groups_z - 1)]
    down = [(b, a) for a, b in up]
    before = lax.ppermute(stacked, "gz", up)
    after = lax.ppermute(stacked, "gz", down)
    spectra = forward(where, own_m, other_m, halves(t["ty"]), halves(t["tz"]))
    own, other = inverse(
        where, spectra, own_m[3], stacked, halves(t["ty_back"]), halves(t["tz_back"]), shares, share
    )
    arrived = lax.ppermute(other, "gy", swap)
    send_f = own + arrived[: 4 * groups_z]
    recv_f = lax.all_to_all(send_f.reshape(groups_z, 4, columns), "gz", 0, 0, tiled=True)
    recv_f = recv_f.reshape(4 * columns, columns)
    tx_back, ny_back = halves(t["tx_back"]), halves(t["ny_back"])
    return finish(where, recv_f, arrived, stacked, before, after, tx_back, ny_back)[:, None]


def solution(mesh):
    placed = (
        P(None, ("parts", "gz"), "gy", None),
        P(("parts", "gz"), "gy", None),
        P(),
        P(None, "gz", "gy", None),
        P(None, "gz", "gy"),
    )

    return jax.shard_map(
        local,
        mesh=mesh,
        in_specs=placed,
        out_specs=P(None, ("parts", "gz"), "gy", None),
        check_vma=False,
    )
```

```python
import jax
import jax.numpy as jnp
import numpy as np
from jax import lax
from jax.experimental import pallas as pl
from jax.experimental.pallas import tpu as pltpu
from jax.sharding import PartitionSpec as P


exchange_stiffness = 0.25
tensor_index = ((0, 3, 4), (3, 1, 5), (4, 5, 2))
swap = [(0, 1), (1, 0)]
bf16 = jnp.bfloat16
f32 = jnp.float32
limits = pltpu.CompilerParams(vmem_limit_bytes=20 * 2**20)


def wave(first, second, period):
    angle = 2.0 * np.pi / period * (np.outer(first, second) % period)
    return np.cos(angle), np.sin(angle)


def slot_frequencies(groups_z):
    bits = groups_z.bit_length() - 1
    reversed_bits = np.array([int(format(d, f"0{bits}b")[::-1], 2) for d in range(groups_z)])
    return np.concatenate([2 * reversed_bits, 2 * reversed_bits + 1])


def tables(columns, rows, groups_z):
    half = rows // 2
    x = np.arange(columns)
    y = np.arange(rows)
    ky = np.arange(2 * rows)
    z = np.arange(groups_z)
    out = {}
    cx, sx = wave(x, x, 2 * columns)
    out["tx"] = np.concatenate([cx, -sx], axis=1)
    forward, back = [], []
    for g in range(2):
        own_ky = ky[g * rows : (g + 1) * rows]
        there, here = [], []
        for h in (g, 1 - g):
            c, s = wave(y[h * half : (h + 1) * half], own_ky, 2 * rows)
            there.append(np.block([[c, -s], [s, c]]))
            here.append(np.block([[c.T, s.T], [-s.T, c.T]]))
        forward.append(np.concatenate(there, axis=0))
        back.append(np.concatenate(here, axis=1))
    out["ty"] = np.stack(forward)
    out["ty_back"] = np.stack(back)
    c, s = wave(slot_frequencies(groups_z), z, 2 * groups_z)
    out["tz"] = np.concatenate([c, s], axis=1)
    out["tz_back"] = np.stack([np.concatenate([t[k * groups_z : (k + 1) * groups_z].T for t in (c, s)], axis=1) for k in range(2)])
    w = np.where(x == 0, 1.0, 2.0)[:, None]
    scale = 1.0 / (2.0 * columns * 2.0 * rows * 2.0 * groups_z)
    out["tx_back"] = np.concatenate([w * cx, -w * sx], axis=1) * scale
    forward, back = [], []
    for g in range(2):
        c, s = wave(ky, y[g * half : (g + 1) * half], 2 * rows)
        c, s = c.reshape(2, rows, half), s.reshape(2, rows, half)
        forward.append(np.concatenate([c[0], -s[0], c[1], -s[1]], axis=1))
        back.append(np.concatenate([c[0].T, -s[0].T, c[1].T, -s[1].T], axis=0) * scale)
    out["ny"] = np.stack(forward)
    out["ny_back"] = np.stack(back)
    return out


def halves(table):
    table = np.asarray(table, dtype=np.float32)
    high = table.astype(bf16)
    low = (table - high.astype(np.float32)).astype(bf16)
    return jnp.asarray(np.stack([high, low]))


def split(x):
    high = x.astype(bf16)
    return high, (x - high.astype(f32)).astype(bf16)


def three(left, right, dims=((1,), (0,))):
    (lh, ll), (rh, rl) = left, right
    prod = lambda a, b: lax.dot_general(a, b, (dims, ((), ())), preferred_element_type=f32)
    return prod(lh, rh) + (prod(lh, rl) + prod(ll, rh))


def cross(real, imag, lower):
    return jnp.concatenate([jnp.concatenate([real, imag], axis=1), lower], axis=0)


def prepare_kernel(slots, mine_ref, sat_hbm, dir_hbm, reg_hbm, main_hbm, nyq_hbm, tx_hbm, ny_hbm,
                   send_ref, stack_ref, sat_ref, dirs, reg, main, nyq, tx, ny, rows_t, sems):
    _, half, columns = dirs.shape
    width = 4 + 6 * slots
    copies = [
        pltpu.make_async_copy(reg_hbm, reg, sems.at[0]),
        pltpu.make_async_copy(dir_hbm, dirs, sems.at[1]),
        pltpu.make_async_copy(main_hbm.at[:, pl.ds(mine_ref[0], slots)], main, sems.at[2]),
        pltpu.make_async_copy(tx_hbm, tx, sems.at[3]),
        pltpu.make_async_copy(ny_hbm.at[mine_ref[1]], ny, sems.at[4]),
        pltpu.make_async_copy(nyq_hbm, nyq, sems.at[5]),
        pltpu.make_async_copy(sat_hbm, sat_ref, sems.at[6]),
    ]
    for c in copies:
        c.start()
    rows_t[...] = jnp.zeros_like(rows_t)
    copies[0].wait()
    region = reg[...]
    magnetic = (region > 0).astype(f32)
    strength = jnp.zeros(region.shape, f32)
    copies[6].wait()
    for r in range(3):
        strength = strength + jnp.where(region == r + 1, sat_ref[r], 0.0)
    copies[1].wait()
    stack_ref[3] = magnetic
    lane = lax.broadcasted_iota(jnp.int32, (half, columns), 1)
    signs = (1 - 2 * (lane % 2)).astype(f32)
    moments = []
    sums = jnp.zeros((half, columns), f32)
    for c in range(3):
        one = dirs[c]
        stack_ref[c] = one * magnetic
        moment = one * strength
        moments.append(moment)
        total = jnp.sum(moment * signs, axis=1, keepdims=True)
        sums = jnp.where((lane % 4 == c) & (lane % 32 < 12), total, sums)
    copies[3].wait()
    zero = jnp.zeros((half, columns), bf16)
    table = (tx[0], tx[1])
    for c in range(3):
        high, low = split(moments[c])
        wide = [jnp.concatenate([jnp.concatenate([p, zero], 1), jnp.concatenate([zero, p], 1)], 0) for p in (high, low)]
        send_ref[pl.ds(c, columns, stride=width), :] = three(table, wide, ((1,), (1,)))
    copies[2].wait()
    for s in range(slots):
        for r in range(6):
            send_ref[pl.ds(4 + 6 * s + r, columns, stride=width), :] = main[r, s].T
    copies[4].wait()
    parts = [split(jnp.where(lane // 32 == q, sums, 0.0)) for q in range(4)]
    stacked = [jnp.concatenate([p[k] for p in parts], axis=0) for k in range(2)]
    row = three((ny[0], ny[1]), stacked)
    copies[5].wait()
    for s in range(2):
        for i in range(3):
            for j in range(3):
                rows_t[pl.ds(64 * s + 16 + 4 * i + j, 1), :] = nyq[tensor_index[i][j], pl.ds(s, 1), :]
    send_ref[pl.ds(3, columns, stride=width), :] = row + rows_t[...].T


def prepare(mine, saturation, direction, region, kernel_main, kernel_nyq, tx, ny, slots):
    _, half, columns = direction.shape
    rows = kernel_main.shape[2]
    any_spec = pl.BlockSpec(memory_space=pltpu.HBM)
    smem = pl.BlockSpec(memory_space=pltpu.SMEM)
    vmem = pl.BlockSpec(memory_space=pltpu.VMEM)

    def body(*refs):
        prepare_kernel(slots, *refs)

    return pl.pallas_call(
        body,
        name="prepare",
        compiler_params=limits,
        out_shape=(
            jax.ShapeDtypeStruct((columns * (4 + 6 * slots), columns), f32),
            jax.ShapeDtypeStruct((4, half, columns), f32),
        ),
        in_specs=[smem] + [any_spec] * 7,
        out_specs=(vmem, vmem),
        scratch_shapes=[
            pltpu.SMEM(saturation.shape, f32),
            pltpu.VMEM((3, half, columns), f32),
            pltpu.VMEM((half, columns), jnp.int32),
            pltpu.VMEM((6, slots, rows, columns), f32),
            pltpu.VMEM(kernel_nyq.shape, f32),
            pltpu.VMEM(tx.shape, bf16),
            pltpu.VMEM(ny.shape[1:], bf16),
            pltpu.VMEM((columns, columns), f32),
            pltpu.SemaphoreType.DMA((7,)),
        ],
    )(mine, *(pltpu.with_memory_space_constraint(a, pltpu.HBM) for a in (saturation, direction, region, kernel_main, kernel_nyq, tx, ny)))


def forward_kernel(where_ref, own, other, ty, tz, out):
    planes, width = own.shape[1:]
    table = (tz[0], tz[1])
    y_table = (ty[0, where_ref[1]], ty[1, where_ref[1]])
    for c in range(4):
        if c < 3:
            ready = three(split(jnp.concatenate([own[c], other[c]], axis=1)), y_table)
            real, imag = ready[:, :width], ready[:, width:]
        else:
            lane = lax.broadcasted_iota(jnp.int32, (planes, width), 1)
            summed = own[3] + other[3]
            summed = jnp.where(where_ref[1] == 0, summed, pltpu.roll(summed, 64, 1))
            real = jnp.where(lane < 12, summed, 0.0)
            imag = jnp.where(lane < 12, pltpu.roll(summed, width - 32, 1), 0.0)
        (rh, rl), (ih, il) = split(real), split(imag)
        crossed = [cross(r, i, jnp.concatenate([i, -r], axis=1)) for r, i in ((rh, ih), (rl, il))]
        done = three(table, crossed)
        out[c, 0] = done[:planes]
        out[c, 1] = done[planes:]


def forward(where, own, other, ty, tz):
    planes, width = own.shape[1:]
    smem = pl.BlockSpec(memory_space=pltpu.SMEM)
    vmem = pl.BlockSpec(memory_space=pltpu.VMEM)
    return pl.pallas_call(
        forward_kernel,
        name="forward",
        compiler_params=limits,
        out_shape=jax.ShapeDtypeStruct((4, 2, planes, 2 * width), f32),
        in_specs=[smem] + [vmem] * 4,
        out_specs=vmem,
    )(where, own, other, ty, tz)


def back(real, imag, table):
    (rh, rl), (ih, il) = split(real), split(imag)
    crossed = [cross(r, i, jnp.concatenate([-i, r], axis=1)) for r, i in ((rh, ih), (rl, il))]
    return three(table, crossed)


def field_of(kernel, spectra, slot, i):
    width = kernel.shape[2]
    real = imag = None
    for j in range(3):
        k = kernel[tensor_index[i][j]]
        a, b = k * spectra[j, slot, :, :width], k * spectra[j, slot, :, width:]
        real, imag = (a, b) if real is None else (real + a, imag + b)
    return real, imag


def first_half_kernel(where_ref, spectra, kernel, row_ref, tz, out, line_out):
    planes, width = row_ref.shape
    slot = where_ref[0]
    table = (tz[0, slot], tz[1, slot])
    for i in range(3):
        out[i] = back(*field_of(kernel, spectra, slot, i), table)
    lane = lax.broadcasted_iota(jnp.int32, (planes, width), 1)
    row = row_ref[...]
    line = jnp.zeros((planes, 2 * width), f32)
    for s in range(2):
        k = jnp.where(lane < 12, pltpu.roll(row, width - 16 - 64 * s, 1), 0.0)
        line = line + back(spectra[3, s, :, :width] * k, spectra[3, s, :, width:] * k, (tz[0, s], tz[1, s]))
    line = line[:, :width] + pltpu.roll(line[:, width:], 32, 1)
    line_out[...] = jnp.where(where_ref[1] == 0, line, pltpu.roll(line, 64, 1))


def first_half(where, spectra, kernel, row, tz):
    planes, width = row.shape
    smem = pl.BlockSpec(memory_space=pltpu.SMEM)
    vmem = pl.BlockSpec(memory_space=pltpu.VMEM)
    return pl.pallas_call(
        first_half_kernel,
        name="first_half",
        compiler_params=limits,
        out_shape=(
            jax.ShapeDtypeStruct((3, planes, 2 * width), f32),
            jax.ShapeDtypeStruct((planes, width), f32),
        ),
        in_specs=[smem] + [vmem] * 4,
        out_specs=(vmem, vmem),
    )(where, spectra, kernel, row, tz)


def second_half_kernel(where_ref, spectra, kernel, ready, line_ref, stack, tz, ty, own, other):
    planes, width = line_ref.shape
    slot = 1 - where_ref[0]
    table = (tz[0, slot], tz[1, slot])
    y_table = (ty[0, where_ref[1]], ty[1, where_ref[1]])
    for i in range(3):
        lines = ready[i] + back(*field_of(kernel, spectra, slot, i), table)
        lines = three(split(lines), y_table)
        own[pl.ds(i, planes, stride=4), :] = lines[:, :width]
        other[pl.ds(i, planes, stride=4), :] = lines[:, width:]
    own[pl.ds(3, planes, stride=4), :] = line_ref[...]
    other[pl.ds(3, planes, stride=4), :] = line_ref[...]
    last = stack.shape[1] - 1
    for c in range(4):
        edge = jnp.where(where_ref[1] == 0, stack[c, last:], stack[c, :1])
        other[4 * planes + c : 4 * planes + c + 1, :] = edge
        other[4 * planes + 4 + c : 4 * planes + 5 + c, :] = edge


def second_half(where, spectra, kernel, ready, line, stacked, tz, ty):
    planes, width = line.shape
    smem = pl.BlockSpec(memory_space=pltpu.SMEM)
    vmem = pl.BlockSpec(memory_space=pltpu.VMEM)
    return pl.pallas_call(
        second_half_kernel,
        name="second_half",
        compiler_params=limits,
        out_shape=(
            jax.ShapeDtypeStruct((4 * planes, width), f32),
            jax.ShapeDtypeStruct((4 * planes + 8, width), f32),
        ),
        in_specs=[smem] + [vmem] * 7,
        out_specs=(vmem, vmem),
    )(where, spectra, kernel, ready, line, stacked, tz, ty)


def finish_kernel(where_ref, recv, arrived, stack, before, after, tx, ny, out):
    _, half, columns = stack.shape
    lane = lax.broadcasted_iota(jnp.int32, (half, columns), 1)
    line = lax.broadcasted_iota(jnp.int32, (half, columns), 0)
    signs = (1 - 2 * (lane % 2)).astype(f32)
    lower = where_ref[1] == 0

    def near(c):
        one = stack[c]
        edge = arrived[pl.ds(4 * columns + c, 1), :]
        low = jnp.where(line == 0, jnp.where(lower, 0.0, edge), pltpu.roll(one, 1, 0))
        high = jnp.where(line == half - 1, jnp.where(lower, edge, 0.0), pltpu.roll(one, half - 1, 0))
        left = jnp.where(lane == 0, 0.0, pltpu.roll(one, 1, 1))
        right = jnp.where(lane == columns - 1, 0.0, pltpu.roll(one, columns - 1, 1))
        return before[c] + after[c] + low + high + left + right

    count = near(3)
    magnetic = stack[3]
    nyquist = three((ny[0, where_ref[1]], ny[1, where_ref[1]]), split(recv[pl.ds(3, columns, stride=4), :]))
    sums = jnp.zeros((half, columns), f32)
    for q in range(4):
        sums = jnp.where(lane // 32 == q, nyquist[q * half : (q + 1) * half], sums)
    table = (tx[0], tx[1])
    for c in range(3):
        prod = three(split(recv[pl.ds(c, columns, stride=4), :].T), table)
        demag = prod[:half, :columns] + prod[half:, columns:]
        total = jnp.sum(jnp.where(lane % 32 // 4 == c, sums, 0.0), axis=1, keepdims=True)
        exchange = exchange_stiffness * (magnetic * near(c) - count * stack[c])
        out[c] = demag + total * signs + exchange


def finish(where, recv, arrived, stacked, before, after, tx, ny):
    smem = pl.BlockSpec(memory_space=pltpu.SMEM)
    vmem = pl.BlockSpec(memory_space=pltpu.VMEM)
    return pl.pallas_call(
        finish_kernel,
        name="finish",
        compiler_params=limits,
        out_shape=jax.ShapeDtypeStruct((3,) + stacked.shape[1:], f32),
        in_specs=[smem] + [vmem] * 7,
        out_specs=vmem,
    )(where, recv, arrived, stacked, before, after, tx, ny)


def local(direction, region, saturation, kernel_main, kernel_nyq):
    columns = direction.shape[3]
    half = direction.shape[2]
    groups_z = lax.axis_size("gz")
    rows = half * lax.axis_size("gy")
    parts = lax.axis_size("parts")
    y_index = lax.axis_index("gy")
    part = lax.axis_index("parts")
    pairs = 2 if parts % 2 == 0 else 1
    slots = 2 // pairs
    t = tables(columns, rows, groups_z)
    direction = direction[:, 0]
    where = jnp.stack([part % pairs, y_index])
    send, stacked = prepare(
        where, saturation, direction, region[0], kernel_main, kernel_nyq,
        halves(t["tx"]), halves(t["ny"]).swapaxes(0, 1), slots,
    )
    width = 4 + 6 * slots
    recv = lax.all_to_all(send.reshape(columns, width // 2, 2, columns), "gz", 0, 0, tiled=True)
    recv = recv.reshape(columns, width, columns).transpose(1, 0, 2)
    kernel = recv[4:10]
    if pairs == 2:
        kernel_other = lax.ppermute(kernel, "parts", [(p, p ^ 1) for p in range(parts)])
    else:
        kernel_other = recv[10:]
    own_m = recv[:4]
    other_m = lax.ppermute(own_m, "gy", swap)
    tz_back = halves(t["tz_back"])
    spectra = forward(where, own_m, other_m, halves(t["ty"]), halves(t["tz"]))
    ready, line = first_half(where, spectra, kernel, own_m[3], tz_back)
    own, other = second_half(where, spectra, kernel_other, ready, line, stacked, tz_back, halves(t["ty_back"]))
    arrived = lax.ppermute(other, "gy", swap)
    send_f = own + arrived[: 4 * groups_z]
    recv_f = lax.all_to_all(send_f.reshape(groups_z, 4, columns), "gz", 0, 0, tiled=True)
    recv_f = recv_f.reshape(4 * columns, columns)
    up = [(i, i + 1) for i in range(groups_z - 1)]
    down = [(b, a) for a, b in up]
    edge_planes, _ = lax.optimization_barrier((stacked, send_f))
    before = lax.ppermute(edge_planes, "gz", up)
    after = lax.ppermute(edge_planes, "gz", down)
    tx_back, ny_back = halves(t["tx_back"]), halves(t["ny_back"])
    return finish(where, recv_f, arrived, stacked, before, after, tx_back, ny_back)[:, None]


def solution(mesh):
    placed = (
        P(None, ("parts", "gz"), "gy", None),
        P(("parts", "gz"), "gy", None),
        P(),
        P(None, "gz", "gy", None),
        P(None, "gz", "gy"),
    )

    return jax.shard_map(
        local,
        mesh=mesh,
        in_specs=placed,
        out_specs=P(None, ("parts", "gz"), "gy", None),
        check_vma=False,
    )
```

```python
import functools

import jax
import jax.numpy as jnp
import numpy as np
from jax import lax
from jax.experimental import pallas as pl
from jax.experimental.pallas import tpu as pltpu
from jax.sharding import PartitionSpec as P


exchange_stiffness = 0.25
tensor_index = ((0, 3, 4), (3, 1, 5), (4, 5, 2))
swap = [(0, 1), (1, 0)]
bf16 = jnp.bfloat16
f32 = jnp.float32
limits = pltpu.CompilerParams(vmem_limit_bytes=20 * 2**20)


def wave(first, second, period):
    angle = 2.0 * np.pi / period * (np.outer(first, second) % period)
    return np.cos(angle), np.sin(angle)


def slot_frequencies(groups_z):
    bits = groups_z.bit_length() - 1
    reversed_bits = np.array([int(format(d, f"0{bits}b")[::-1], 2) for d in range(groups_z)])
    return np.concatenate([2 * reversed_bits, 2 * reversed_bits + 1])


def tables(columns, rows, groups_z):
    half = rows // 2
    x = np.arange(columns)
    y = np.arange(rows)
    ky = np.arange(2 * rows)
    z = np.arange(groups_z)
    out = {}
    cx, sx = wave(x, x, 2 * columns)
    out["tx"] = np.concatenate([cx, -sx], axis=1)
    forward, back = [], []
    for g in range(2):
        own_ky = ky[g * rows : (g + 1) * rows]
        there, here = [], []
        for h in (g, 1 - g):
            c, s = wave(y[h * half : (h + 1) * half], own_ky, 2 * rows)
            there.append(np.block([[c, -s], [s, c]]))
            here.append(np.block([[c.T, s.T], [-s.T, c.T]]))
        forward.append(np.concatenate(there, axis=0))
        back.append(np.concatenate(here, axis=1))
    out["ty"] = np.stack(forward)
    out["ty_back"] = np.stack(back)
    c, s = wave(slot_frequencies(groups_z), z, 2 * groups_z)
    out["tz"] = np.concatenate([c, s], axis=1)
    out["tz_back"] = np.stack([np.concatenate([t[k * groups_z : (k + 1) * groups_z].T for t in (c, s)], axis=1) for k in range(2)])
    w = np.where(x == 0, 1.0, 2.0)[:, None]
    scale = 1.0 / (2.0 * columns * 2.0 * rows * 2.0 * groups_z)
    out["tx_back"] = np.concatenate([w * cx, -w * sx], axis=1) * scale
    forward, back = [], []
    for g in range(2):
        c, s = wave(ky, y[g * half : (g + 1) * half], 2 * rows)
        c, s = c.reshape(2, rows, half), s.reshape(2, rows, half)
        forward.append(np.concatenate([c[0], -s[0], c[1], -s[1]], axis=1))
        back.append(np.concatenate([c[0].T, -s[0].T, c[1].T, -s[1].T], axis=0) * scale)
    out["ny"] = np.stack(forward)
    out["ny_back"] = np.stack(back)
    return out


def halves(table):
    table = np.asarray(table, dtype=np.float32)
    high = table.astype(bf16)
    low = (table - high.astype(np.float32)).astype(bf16)
    return jnp.asarray(np.stack([high, low]))


def split(x):
    high = x.astype(bf16)
    return high, (x - high.astype(f32)).astype(bf16)


def three(left, right, dims=((1,), (0,))):
    (lh, ll), (rh, rl) = left, right
    prod = lambda a, b: lax.dot_general(a, b, (dims, ((), ())), preferred_element_type=f32)
    return prod(lh, rh) + (prod(lh, rl) + prod(ll, rh))


def cross(real, imag, lower):
    return jnp.concatenate([jnp.concatenate([real, imag], axis=1), lower], axis=0)


def place(axis, count):
    return lax.rem(lax.axis_index(axis), count)


def prepare_kernel(slots, sat_hbm, dir_hbm, reg_hbm, main_hbm, nyq_hbm, tx_hbm, ny_hbm,
                   send_ref, stack_ref, sat_ref, dirs, reg, main, nyq, tx, ny, rows_t, sems):
    _, half, columns = dirs.shape
    width = 4 + 6 * slots
    slot = place("parts", 2 // slots)
    copies = [
        pltpu.make_async_copy(reg_hbm, reg, sems.at[0]),
        pltpu.make_async_copy(dir_hbm, dirs, sems.at[1]),
        pltpu.make_async_copy(main_hbm.at[:, pl.ds(slot, slots)], main, sems.at[2]),
        pltpu.make_async_copy(tx_hbm, tx, sems.at[3]),
        pltpu.make_async_copy(ny_hbm.at[place("gy", 2)], ny, sems.at[4]),
        pltpu.make_async_copy(nyq_hbm, nyq, sems.at[5]),
        pltpu.make_async_copy(sat_hbm, sat_ref, sems.at[6]),
    ]
    for c in copies:
        c.start()
    rows_t[...] = jnp.zeros_like(rows_t)
    copies[0].wait()
    region = reg[...]
    magnetic = (region > 0).astype(f32)
    strength = jnp.zeros(region.shape, f32)
    copies[6].wait()
    for r in range(3):
        strength = strength + jnp.where(region == r + 1, sat_ref[r], 0.0)
    copies[1].wait()
    stack_ref[3] = magnetic
    lane = lax.broadcasted_iota(jnp.int32, (half, columns), 1)
    signs = (1 - 2 * (lane % 2)).astype(f32)
    moments = []
    sums = jnp.zeros((half, columns), f32)
    for c in range(3):
        one = dirs[c]
        stack_ref[c] = one * magnetic
        moment = one * strength
        moments.append(moment)
        total = jnp.sum(moment * signs, axis=1, keepdims=True)
        sums = jnp.where((lane % 4 == c) & (lane % 32 < 12), total, sums)
    copies[3].wait()
    zero = jnp.zeros((half, columns), bf16)
    table = (tx[0], tx[1])
    for c in range(3):
        high, low = split(moments[c])
        wide = [jnp.concatenate([jnp.concatenate([p, zero], 1), jnp.concatenate([zero, p], 1)], 0) for p in (high, low)]
        send_ref[pl.ds(c, columns, stride=width), :] = three(table, wide, ((1,), (1,)))
    copies[2].wait()
    for s in range(slots):
        for r in range(6):
            send_ref[pl.ds(4 + 6 * s + r, columns, stride=width), :] = main[r, s].T
    copies[4].wait()
    parts = [split(jnp.where(lane // 32 == q, sums, 0.0)) for q in range(4)]
    stacked = [jnp.concatenate([p[k] for p in parts], axis=0) for k in range(2)]
    row = three((ny[0], ny[1]), stacked)
    copies[5].wait()
    for s in range(2):
        for i in range(3):
            for j in range(3):
                rows_t[pl.ds(64 * s + 16 + 4 * i + j, 1), :] = nyq[tensor_index[i][j], pl.ds(s, 1), :]
    send_ref[pl.ds(3, columns, stride=width), :] = row + rows_t[...].T


def prepare(saturation, direction, region, kernel_main, kernel_nyq, tx, ny, slots):
    _, half, columns = direction.shape
    rows = kernel_main.shape[2]
    any_spec = pl.BlockSpec(memory_space=pltpu.HBM)
    vmem = pl.BlockSpec(memory_space=pltpu.VMEM)

    return pl.pallas_call(
        functools.partial(prepare_kernel, slots),
        name="prepare",
        compiler_params=limits,
        out_shape=(
            jax.ShapeDtypeStruct((columns * (4 + 6 * slots), columns), f32),
            jax.ShapeDtypeStruct((4, half, columns), f32),
        ),
        in_specs=[any_spec] * 7,
        out_specs=(vmem, vmem),
        scratch_shapes=[
            pltpu.SMEM(saturation.shape, f32),
            pltpu.VMEM((3, half, columns), f32),
            pltpu.VMEM((half, columns), jnp.int32),
            pltpu.VMEM((6, slots, rows, columns), f32),
            pltpu.VMEM(kernel_nyq.shape, f32),
            pltpu.VMEM(tx.shape, bf16),
            pltpu.VMEM(ny.shape[1:], bf16),
            pltpu.VMEM((columns, columns), f32),
            pltpu.SemaphoreType.DMA((7,)),
        ],
    )(*(pltpu.with_memory_space_constraint(a, pltpu.HBM) for a in (saturation, direction, region, kernel_main, kernel_nyq, tx, ny)))


def forward_kernel(own, other, ty, tz, out):
    planes, width = own.shape[1:]
    gy = place("gy", 2)
    table = (tz[0], tz[1])
    y_table = (ty[0, gy], ty[1, gy])
    for c in range(4):
        if c < 3:
            ready = three(split(jnp.concatenate([own[c], other[c]], axis=1)), y_table)
            real, imag = ready[:, :width], ready[:, width:]
        else:
            lane = lax.broadcasted_iota(jnp.int32, (planes, width), 1)
            summed = own[3] + other[3]
            summed = jnp.where(place("gy", 2) == 0, summed, pltpu.roll(summed, 64, 1))
            real = jnp.where(lane < 12, summed, 0.0)
            imag = jnp.where(lane < 12, pltpu.roll(summed, width - 32, 1), 0.0)
        (rh, rl), (ih, il) = split(real), split(imag)
        crossed = [cross(r, i, jnp.concatenate([i, -r], axis=1)) for r, i in ((rh, ih), (rl, il))]
        done = three(table, crossed)
        out[c, 0] = done[:planes]
        out[c, 1] = done[planes:]


def forward(own, other, ty, tz):
    planes, width = own.shape[1:]
    vmem = pl.BlockSpec(memory_space=pltpu.VMEM)
    return pl.pallas_call(
        forward_kernel,
        name="forward",
        compiler_params=limits,
        out_shape=jax.ShapeDtypeStruct((4, 2, planes, 2 * width), f32),
        in_specs=[vmem] * 4,
        out_specs=vmem,
    )(own, other, ty, tz)


def back(real, imag, table):
    (rh, rl), (ih, il) = split(real), split(imag)
    crossed = [cross(r, i, jnp.concatenate([-i, r], axis=1)) for r, i in ((rh, ih), (rl, il))]
    return three(table, crossed)


def field_of(kernel, spectra, slot, i):
    width = kernel.shape[2]
    real = imag = None
    for j in range(3):
        k = kernel[tensor_index[i][j]]
        a, b = k * spectra[j, slot, :, :width], k * spectra[j, slot, :, width:]
        real, imag = (a, b) if real is None else (real + a, imag + b)
    return real, imag


def first_half_kernel(pairs, spectra, kernel, row_ref, tz, out, line_out):
    planes, width = row_ref.shape
    slot = place("parts", pairs)
    table = (tz[0, slot], tz[1, slot])
    for i in range(3):
        out[i] = back(*field_of(kernel, spectra, slot, i), table)
    lane = lax.broadcasted_iota(jnp.int32, (planes, width), 1)
    row = row_ref[...]
    line = jnp.zeros((planes, 2 * width), f32)
    for s in range(2):
        k = jnp.where(lane < 12, pltpu.roll(row, width - 16 - 64 * s, 1), 0.0)
        line = line + back(spectra[3, s, :, :width] * k, spectra[3, s, :, width:] * k, (tz[0, s], tz[1, s]))
    line = line[:, :width] + pltpu.roll(line[:, width:], 32, 1)
    line_out[...] = jnp.where(place("gy", 2) == 0, line, pltpu.roll(line, 64, 1))


def first_half(pairs, spectra, kernel, row, tz):
    planes, width = row.shape
    vmem = pl.BlockSpec(memory_space=pltpu.VMEM)
    return pl.pallas_call(
        functools.partial(first_half_kernel, pairs),
        name="first_half",
        compiler_params=limits,
        out_shape=(
            jax.ShapeDtypeStruct((3, planes, 2 * width), f32),
            jax.ShapeDtypeStruct((planes, width), f32),
        ),
        in_specs=[vmem] * 4,
        out_specs=(vmem, vmem),
    )(spectra, kernel, row, tz)


def second_half_kernel(pairs, spectra, kernel, ready, line_ref, stack, tz, ty, own, other):
    planes, width = line_ref.shape
    slot = 1 - place("parts", pairs)
    gy = place("gy", 2)
    table = (tz[0, slot], tz[1, slot])
    y_table = (ty[0, gy], ty[1, gy])
    for i in range(3):
        lines = ready[i] + back(*field_of(kernel, spectra, slot, i), table)
        lines = three(split(lines), y_table)
        own[pl.ds(i, planes, stride=4), :] = lines[:, :width]
        other[pl.ds(i, planes, stride=4), :] = lines[:, width:]
    own[pl.ds(3, planes, stride=4), :] = line_ref[...]
    other[pl.ds(3, planes, stride=4), :] = line_ref[...]
    last = stack.shape[1] - 1
    for c in range(4):
        edge = jnp.where(place("gy", 2) == 0, stack[c, last:], stack[c, :1])
        other[4 * planes + c : 4 * planes + c + 1, :] = edge
        other[4 * planes + 4 + c : 4 * planes + 5 + c, :] = edge


def second_half(pairs, spectra, kernel, ready, line, stacked, tz, ty):
    planes, width = line.shape
    vmem = pl.BlockSpec(memory_space=pltpu.VMEM)
    return pl.pallas_call(
        functools.partial(second_half_kernel, pairs),
        name="second_half",
        compiler_params=limits,
        out_shape=(
            jax.ShapeDtypeStruct((4 * planes, width), f32),
            jax.ShapeDtypeStruct((4 * planes + 8, width), f32),
        ),
        in_specs=[vmem] * 7,
        out_specs=(vmem, vmem),
    )(spectra, kernel, ready, line, stacked, tz, ty)


def finish_kernel(recv, arrived, stack, before, after, tx, ny, out):
    _, half, columns = stack.shape
    lane = lax.broadcasted_iota(jnp.int32, (half, columns), 1)
    line = lax.broadcasted_iota(jnp.int32, (half, columns), 0)
    signs = (1 - 2 * (lane % 2)).astype(f32)
    gy = place("gy", 2)
    lower = gy == 0

    def near(c):
        one = stack[c]
        edge = arrived[pl.ds(4 * columns + c, 1), :]
        low = jnp.where(line == 0, jnp.where(lower, 0.0, edge), pltpu.roll(one, 1, 0))
        high = jnp.where(line == half - 1, jnp.where(lower, edge, 0.0), pltpu.roll(one, half - 1, 0))
        left = jnp.where(lane == 0, 0.0, pltpu.roll(one, 1, 1))
        right = jnp.where(lane == columns - 1, 0.0, pltpu.roll(one, columns - 1, 1))
        return before[c] + after[c] + low + high + left + right

    count = near(3)
    magnetic = stack[3]
    nyquist = three((ny[0, gy], ny[1, gy]), split(recv[pl.ds(3, columns, stride=4), :]))
    sums = jnp.zeros((half, columns), f32)
    for q in range(4):
        sums = jnp.where(lane // 32 == q, nyquist[q * half : (q + 1) * half], sums)
    table = (tx[0], tx[1])
    for c in range(3):
        prod = three(split(recv[pl.ds(c, columns, stride=4), :].T), table)
        demag = prod[:half, :columns] + prod[half:, columns:]
        total = jnp.sum(jnp.where(lane % 32 // 4 == c, sums, 0.0), axis=1, keepdims=True)
        exchange = exchange_stiffness * (magnetic * near(c) - count * stack[c])
        out[c] = demag + total * signs + exchange


def finish(recv, arrived, stacked, before, after, tx, ny):
    vmem = pl.BlockSpec(memory_space=pltpu.VMEM)
    return pl.pallas_call(
        finish_kernel,
        name="finish",
        compiler_params=limits,
        out_shape=jax.ShapeDtypeStruct((3,) + stacked.shape[1:], f32),
        in_specs=[vmem] * 7,
        out_specs=vmem,
    )(recv, arrived, stacked, before, after, tx, ny)


def local(direction, region, saturation, kernel_main, kernel_nyq):
    columns = direction.shape[3]
    half = direction.shape[2]
    groups_z = lax.axis_size("gz")
    rows = half * lax.axis_size("gy")
    parts = lax.axis_size("parts")
    pairs = 2 if parts % 2 == 0 else 1
    slots = 2 // pairs
    t = tables(columns, rows, groups_z)
    direction = direction[:, 0]
    send, stacked = prepare(
        saturation, direction, region[0], kernel_main, kernel_nyq,
        halves(t["tx"]), halves(t["ny"]).swapaxes(0, 1), slots,
    )
    width = 4 + 6 * slots
    up = [(i, i + 1) for i in range(groups_z - 1)]
    down = [(b, a) for a, b in up]
    before = lax.ppermute(stacked, "gz", up)
    after = lax.ppermute(stacked, "gz", down)
    recv = lax.all_to_all(send.reshape(columns, width // 2, 2, columns), "gz", 0, 0, tiled=True)
    recv = recv.reshape(columns, width, columns).transpose(1, 0, 2)
    kernel = recv[4:10]
    if pairs == 2:
        kernel_other = lax.ppermute(kernel, "parts", [(p, p ^ 1) for p in range(parts)])
    else:
        kernel_other = recv[10:]
    own_m = recv[:4]
    other_m = lax.ppermute(own_m, "gy", swap)
    tz_back = halves(t["tz_back"])
    spectra = forward(own_m, other_m, halves(t["ty"]), halves(t["tz"]))
    ready, line = first_half(pairs, spectra, kernel, own_m[3], tz_back)
    own, other = second_half(pairs, spectra, kernel_other, ready, line, stacked, tz_back, halves(t["ty_back"]))
    other, before, after = lax.optimization_barrier((other, before, after))
    arrived = lax.ppermute(other, "gy", swap)
    send_f = own + arrived[: 4 * groups_z]
    recv_f = lax.all_to_all(send_f.reshape(groups_z, 4, columns), "gz", 0, 0, tiled=True)
    recv_f = recv_f.reshape(4 * columns, columns)
    tx_back, ny_back = halves(t["tx_back"]), halves(t["ny_back"])
    return finish(recv_f, arrived, stacked, before, after, tx_back, ny_back)[:, None]


def solution(mesh):
    placed = (
        P(None, ("parts", "gz"), "gy", None),
        P(("parts", "gz"), "gy", None),
        P(),
        P(None, "gz", "gy", None),
        P(None, "gz", "gy"),
    )

    return jax.shard_map(
        local,
        mesh=mesh,
        in_specs=placed,
        out_specs=P(None, ("parts", "gz"), "gy", None),
        check_vma=False,
    )
```

```python
import functools

import jax
import jax.numpy as jnp
import numpy as np
from jax import lax
from jax.experimental import pallas as pl
from jax.experimental.pallas import tpu as pltpu
from jax.sharding import PartitionSpec as P


exchange_stiffness = 0.25
tensor_index = ((0, 3, 4), (3, 1, 5), (4, 5, 2))
swap = [(0, 1), (1, 0)]
bf16 = jnp.bfloat16
f32 = jnp.float32
limits = pltpu.CompilerParams(vmem_limit_bytes=20 * 2**20)


def wave(first, second, period):
    angle = 2.0 * np.pi / period * (np.outer(first, second) % period)
    return np.cos(angle), np.sin(angle)


def slot_frequencies(groups_z):
    bits = groups_z.bit_length() - 1
    reversed_bits = np.array([int(format(d, f"0{bits}b")[::-1], 2) for d in range(groups_z)])
    return np.concatenate([2 * reversed_bits, 2 * reversed_bits + 1])


def tables(columns, rows, groups_z):
    half = rows // 2
    x = np.arange(columns)
    y = np.arange(rows)
    ky = np.arange(2 * rows)
    z = np.arange(groups_z)
    out = {}
    cx, sx = wave(x, x, 2 * columns)
    out["tx"] = np.concatenate([cx, -sx], axis=1)
    forward, back = [], []
    for g in range(2):
        own_ky = ky[g * rows : (g + 1) * rows]
        there, here = [], []
        for h in (g, 1 - g):
            c, s = wave(y[h * half : (h + 1) * half], own_ky, 2 * rows)
            there.append(np.block([[c, -s], [s, c]]))
            here.append(np.block([[c.T, s.T], [-s.T, c.T]]))
        forward.append(np.concatenate(there, axis=0))
        back.append(np.concatenate(here, axis=1))
    out["ty"] = np.stack(forward)
    out["ty_back"] = np.stack(back)
    c, s = wave(slot_frequencies(groups_z), z, 2 * groups_z)
    out["tz"] = np.concatenate([c, s], axis=1)
    out["tz_back"] = np.stack([np.concatenate([t[k * groups_z : (k + 1) * groups_z].T for t in (c, s)], axis=1) for k in range(2)])
    w = np.where(x == 0, 1.0, 2.0)[:, None]
    scale = 1.0 / (2.0 * columns * 2.0 * rows * 2.0 * groups_z)
    out["tx_back"] = np.concatenate([w * cx, -w * sx], axis=1) * scale
    forward, back = [], []
    for g in range(2):
        c, s = wave(ky, y[g * half : (g + 1) * half], 2 * rows)
        c, s = c.reshape(2, rows, half), s.reshape(2, rows, half)
        forward.append(np.concatenate([c[0], -s[0], c[1], -s[1]], axis=1))
        back.append(np.concatenate([c[0].T, -s[0].T, c[1].T, -s[1].T], axis=0) * scale)
    out["ny"] = np.stack(forward)
    out["ny_back"] = np.stack(back)
    return out


def halves(table):
    table = np.asarray(table, dtype=np.float32)
    high = table.astype(bf16)
    low = (table - high.astype(np.float32)).astype(bf16)
    return jnp.asarray(np.stack([high, low]))


def split(x):
    high = x.astype(bf16)
    return high, (x - high.astype(f32)).astype(bf16)


def three(left, right, dims=((1,), (0,))):
    (lh, ll), (rh, rl) = left, right
    prod = lambda a, b: lax.dot_general(a, b, (dims, ((), ())), preferred_element_type=f32)
    return prod(lh, rh) + (prod(lh, rl) + prod(ll, rh))


def cross(real, imag, lower):
    return jnp.concatenate([jnp.concatenate([real, imag], axis=1), lower], axis=0)


def place(axis, count):
    return lax.rem(lax.axis_index(axis), count)


def prepare_kernel(slots, sat_hbm, dir_hbm, reg_hbm, main_hbm, nyq_hbm, tx_hbm, ny_hbm,
                   send_ref, stack_ref, sat_ref, dirs, reg, main, nyq, tx, ny, rows_t, sems):
    _, half, columns = dirs.shape
    width = 4 + 6 * slots
    slot = place("parts", 2 // slots)
    small = [
        pltpu.make_async_copy(sat_hbm, sat_ref, sems.at[0]),
        pltpu.make_async_copy(reg_hbm, reg, sems.at[1]),
        pltpu.make_async_copy(dir_hbm, dirs, sems.at[2]),
        pltpu.make_async_copy(tx_hbm, tx, sems.at[3]),
        pltpu.make_async_copy(nyq_hbm, nyq, sems.at[4]),
        pltpu.make_async_copy(ny_hbm.at[place("gy", 2)], ny, sems.at[5]),
    ]
    lines = [pltpu.make_async_copy(main_hbm.at[r, pl.ds(slot, slots)], main.at[r], sems.at[6 + r]) for r in range(6)]
    for c in small[:3] + lines + small[3:]:
        c.start()
    rows_t[...] = jnp.zeros_like(rows_t)
    for c in small[:3]:
        c.wait()
    region = reg[...]
    magnetic = (region > 0).astype(f32)
    strength = jnp.zeros(region.shape, f32)
    for r in range(3):
        strength = strength + jnp.where(region == r + 1, sat_ref[r], 0.0)
    stack_ref[3] = magnetic
    lane = lax.broadcasted_iota(jnp.int32, (half, columns), 1)
    signs = (1 - 2 * (lane % 2)).astype(f32)
    moments = []
    sums = jnp.zeros((half, columns), f32)
    for c in range(3):
        one = dirs[c]
        stack_ref[c] = one * magnetic
        moment = one * strength
        moments.append(moment)
        total = jnp.sum(moment * signs, axis=1, keepdims=True)
        sums = jnp.where((lane % 4 == c) & (lane % 32 < 12), total, sums)
    for r in range(6):
        lines[r].wait()
        for s in range(slots):
            send_ref[pl.ds(4 + 6 * s + r, columns, stride=width), :] = main[r, s].T
    small[3].wait()
    zero = jnp.zeros((half, columns), bf16)
    table = (tx[0], tx[1])
    for c in range(3):
        high, low = split(moments[c])
        wide = [jnp.concatenate([jnp.concatenate([p, zero], 1), jnp.concatenate([zero, p], 1)], 0) for p in (high, low)]
        send_ref[pl.ds(c, columns, stride=width), :] = three(table, wide, ((1,), (1,)))
    small[4].wait()
    for s in range(2):
        for i in range(3):
            for j in range(3):
                rows_t[pl.ds(64 * s + 16 + 4 * i + j, 1), :] = nyq[tensor_index[i][j], pl.ds(s, 1), :]
    small[5].wait()
    parts = [split(jnp.where(lane // 32 == q, sums, 0.0)) for q in range(4)]
    stacked = [jnp.concatenate([p[k] for p in parts], axis=0) for k in range(2)]
    row = three((ny[0], ny[1]), stacked)
    send_ref[pl.ds(3, columns, stride=width), :] = row + rows_t[...].T


def prepare(saturation, direction, region, kernel_main, kernel_nyq, tx, ny, slots):
    _, half, columns = direction.shape
    rows = kernel_main.shape[2]
    any_spec = pl.BlockSpec(memory_space=pltpu.HBM)
    vmem = pl.BlockSpec(memory_space=pltpu.VMEM)

    return pl.pallas_call(
        functools.partial(prepare_kernel, slots),
        name="prepare",
        compiler_params=limits,
        out_shape=(
            jax.ShapeDtypeStruct((columns * (4 + 6 * slots), columns), f32),
            jax.ShapeDtypeStruct((4, half, columns), f32),
        ),
        in_specs=[any_spec] * 7,
        out_specs=(vmem, vmem),
        scratch_shapes=[
            pltpu.SMEM(saturation.shape, f32),
            pltpu.VMEM((3, half, columns), f32),
            pltpu.VMEM((half, columns), jnp.int32),
            pltpu.VMEM((6, slots, rows, columns), f32),
            pltpu.VMEM(kernel_nyq.shape, f32),
            pltpu.VMEM(tx.shape, bf16),
            pltpu.VMEM(ny.shape[1:], bf16),
            pltpu.VMEM((columns, columns), f32),
            pltpu.SemaphoreType.DMA((12,)),
        ],
    )(*(pltpu.with_memory_space_constraint(a, pltpu.HBM) for a in (saturation, direction, region, kernel_main, kernel_nyq, tx, ny)))


def forward_kernel(own, other, ty, tz, out):
    planes, width = own.shape[1:]
    gy = place("gy", 2)
    table = (tz[0], tz[1])
    y_table = (ty[0, gy], ty[1, gy])
    for c in range(4):
        if c < 3:
            ready = three(split(jnp.concatenate([own[c], other[c]], axis=1)), y_table)
            real, imag = ready[:, :width], ready[:, width:]
        else:
            lane = lax.broadcasted_iota(jnp.int32, (planes, width), 1)
            summed = own[3] + other[3]
            summed = jnp.where(place("gy", 2) == 0, summed, pltpu.roll(summed, 64, 1))
            real = jnp.where(lane < 12, summed, 0.0)
            imag = jnp.where(lane < 12, pltpu.roll(summed, width - 32, 1), 0.0)
        (rh, rl), (ih, il) = split(real), split(imag)
        crossed = [cross(r, i, jnp.concatenate([i, -r], axis=1)) for r, i in ((rh, ih), (rl, il))]
        done = three(table, crossed)
        out[c, 0] = done[:planes]
        out[c, 1] = done[planes:]


def forward(own, other, ty, tz):
    planes, width = own.shape[1:]
    vmem = pl.BlockSpec(memory_space=pltpu.VMEM)
    return pl.pallas_call(
        forward_kernel,
        name="forward",
        compiler_params=limits,
        out_shape=jax.ShapeDtypeStruct((4, 2, planes, 2 * width), f32),
        in_specs=[vmem] * 4,
        out_specs=vmem,
    )(own, other, ty, tz)


def back(real, imag, table):
    (rh, rl), (ih, il) = split(real), split(imag)
    crossed = [cross(r, i, jnp.concatenate([-i, r], axis=1)) for r, i in ((rh, ih), (rl, il))]
    return three(table, crossed)


def field_of(kernel, spectra, slot, i):
    width = kernel.shape[2]
    real = imag = None
    for j in range(3):
        k = kernel[tensor_index[i][j]]
        a, b = k * spectra[j, slot, :, :width], k * spectra[j, slot, :, width:]
        real, imag = (a, b) if real is None else (real + a, imag + b)
    return real, imag


def first_half_kernel(pairs, spectra, kernel, row_ref, tz, out, line_out):
    planes, width = row_ref.shape
    slot = place("parts", pairs)
    table = (tz[0, slot], tz[1, slot])
    for i in range(3):
        out[i] = back(*field_of(kernel, spectra, slot, i), table)
    lane = lax.broadcasted_iota(jnp.int32, (planes, width), 1)
    row = row_ref[...]
    line = jnp.zeros((planes, 2 * width), f32)
    for s in range(2):
        k = jnp.where(lane < 12, pltpu.roll(row, width - 16 - 64 * s, 1), 0.0)
        line = line + back(spectra[3, s, :, :width] * k, spectra[3, s, :, width:] * k, (tz[0, s], tz[1, s]))
    line = line[:, :width] + pltpu.roll(line[:, width:], 32, 1)
    line_out[...] = jnp.where(place("gy", 2) == 0, line, pltpu.roll(line, 64, 1))


def first_half(pairs, spectra, kernel, row, tz):
    planes, width = row.shape
    vmem = pl.BlockSpec(memory_space=pltpu.VMEM)
    return pl.pallas_call(
        functools.partial(first_half_kernel, pairs),
        name="first_half",
        compiler_params=limits,
        out_shape=(
            jax.ShapeDtypeStruct((3, planes, 2 * width), f32),
            jax.ShapeDtypeStruct((planes, width), f32),
        ),
        in_specs=[vmem] * 4,
        out_specs=(vmem, vmem),
    )(spectra, kernel, row, tz)


def second_half_kernel(pairs, spectra, kernel, ready, line_ref, stack, tz, ty, own, other):
    planes, width = line_ref.shape
    slot = 1 - place("parts", pairs)
    gy = place("gy", 2)
    table = (tz[0, slot], tz[1, slot])
    y_table = (ty[0, gy], ty[1, gy])
    for i in range(3):
        lines = ready[i] + back(*field_of(kernel, spectra, slot, i), table)
        lines = three(split(lines), y_table)
        own[pl.ds(i, planes, stride=4), :] = lines[:, :width]
        other[pl.ds(i, planes, stride=4), :] = lines[:, width:]
    own[pl.ds(3, planes, stride=4), :] = line_ref[...]
    other[pl.ds(3, planes, stride=4), :] = line_ref[...]
    last = stack.shape[1] - 1
    for c in range(4):
        edge = jnp.where(place("gy", 2) == 0, stack[c, last:], stack[c, :1])
        other[4 * planes + c : 4 * planes + c + 1, :] = edge
        other[4 * planes + 4 + c : 4 * planes + 5 + c, :] = edge


def second_half(pairs, spectra, kernel, ready, line, stacked, tz, ty):
    planes, width = line.shape
    vmem = pl.BlockSpec(memory_space=pltpu.VMEM)
    return pl.pallas_call(
        functools.partial(second_half_kernel, pairs),
        name="second_half",
        compiler_params=limits,
        out_shape=(
            jax.ShapeDtypeStruct((4 * planes, width), f32),
            jax.ShapeDtypeStruct((4 * planes + 8, width), f32),
        ),
        in_specs=[vmem] * 7,
        out_specs=(vmem, vmem),
    )(spectra, kernel, ready, line, stacked, tz, ty)


def total_kernel(own, arrived, out, ready, sems):
    count = sems.shape[0]
    size = own.shape[0] // count
    copies = []
    for k in range(count):
        piece = pl.ds(k * size, size)
        ready[piece, :] = own[piece, :] + arrived[piece, :]
        copies.append(pltpu.make_async_copy(ready.at[piece], out.at[piece], sems.at[k]))
        copies[-1].start()
    for c in copies:
        c.wait()


def total(own, arrived):
    vmem = pl.BlockSpec(memory_space=pltpu.VMEM)
    return pl.pallas_call(
        total_kernel,
        name="total",
        compiler_params=limits,
        out_shape=jax.ShapeDtypeStruct(own.shape, f32),
        in_specs=[vmem] * 2,
        out_specs=pl.BlockSpec(memory_space=pltpu.HBM),
        scratch_shapes=[pltpu.VMEM(own.shape, f32), pltpu.SemaphoreType.DMA((4,))],
    )(own, arrived)


def finish_kernel(recv, arrived, stack, before, after, tx, ny, out, ready, sems):
    _, half, columns = stack.shape
    lane = lax.broadcasted_iota(jnp.int32, (half, columns), 1)
    line = lax.broadcasted_iota(jnp.int32, (half, columns), 0)
    signs = (1 - 2 * (lane % 2)).astype(f32)
    gy = place("gy", 2)
    lower = gy == 0

    def near(c):
        one = stack[c]
        edge = arrived[pl.ds(4 * columns + c, 1), :]
        low = jnp.where(line == 0, jnp.where(lower, 0.0, edge), pltpu.roll(one, 1, 0))
        high = jnp.where(line == half - 1, jnp.where(lower, edge, 0.0), pltpu.roll(one, half - 1, 0))
        left = jnp.where(lane == 0, 0.0, pltpu.roll(one, 1, 1))
        right = jnp.where(lane == columns - 1, 0.0, pltpu.roll(one, columns - 1, 1))
        return before[c] + after[c] + low + high + left + right

    count = near(3)
    magnetic = stack[3]
    nyquist = three((ny[0, gy], ny[1, gy]), split(recv[pl.ds(3, columns, stride=4), :]))
    sums = jnp.zeros((half, columns), f32)
    for q in range(4):
        sums = jnp.where(lane // 32 == q, nyquist[q * half : (q + 1) * half], sums)
    table = (tx[0], tx[1])
    copies = []
    for c in range(3):
        prod = three(split(recv[pl.ds(c, columns, stride=4), :].T), table)
        demag = prod[:half, :columns] + prod[half:, columns:]
        line_sum = jnp.sum(jnp.where(lane % 32 // 4 == c, sums, 0.0), axis=1, keepdims=True)
        exchange = exchange_stiffness * (magnetic * near(c) - count * stack[c])
        ready[c] = demag + line_sum * signs + exchange
        copies.append(pltpu.make_async_copy(ready.at[c], out.at[c], sems.at[c]))
        copies[-1].start()
    for c in copies:
        c.wait()


def finish(recv, arrived, stacked, before, after, tx, ny):
    vmem = pl.BlockSpec(memory_space=pltpu.VMEM)
    return pl.pallas_call(
        finish_kernel,
        name="finish",
        compiler_params=limits,
        out_shape=jax.ShapeDtypeStruct((3,) + stacked.shape[1:], f32),
        in_specs=[vmem] * 7,
        out_specs=pl.BlockSpec(memory_space=pltpu.HBM),
        scratch_shapes=[pltpu.VMEM((3,) + stacked.shape[1:], f32), pltpu.SemaphoreType.DMA((3,))],
    )(recv, arrived, stacked, before, after, tx, ny)


def local(direction, region, saturation, kernel_main, kernel_nyq):
    columns = direction.shape[3]
    half = direction.shape[2]
    groups_z = lax.axis_size("gz")
    rows = half * lax.axis_size("gy")
    parts = lax.axis_size("parts")
    pairs = 2 if parts % 2 == 0 else 1
    slots = 2 // pairs
    t = tables(columns, rows, groups_z)
    direction = direction[:, 0]
    send, stacked = prepare(
        saturation, direction, region[0], kernel_main, kernel_nyq,
        halves(t["tx"]), halves(t["ny"]).swapaxes(0, 1), slots,
    )
    width = 4 + 6 * slots
    recv = lax.all_to_all(send.reshape(columns, width // 2, 2, columns), "gz", 0, 0, tiled=True)
    recv = recv.reshape(columns, width, columns).transpose(1, 0, 2)
    kernel = recv[4:10]
    if pairs == 2:
        kernel_other = lax.ppermute(kernel, "parts", [(p, p ^ 1) for p in range(parts)])
    else:
        kernel_other = recv[10:]
    own_m = recv[:4]
    other_m = lax.ppermute(own_m, "gy", swap)
    tz_back = halves(t["tz_back"])
    spectra = forward(own_m, other_m, halves(t["ty"]), halves(t["tz"]))
    ready, line = first_half(pairs, spectra, kernel, own_m[3], tz_back)
    own, other = second_half(pairs, spectra, kernel_other, ready, line, stacked, tz_back, halves(t["ty_back"]))
    arrived = lax.ppermute(other, "gy", swap)
    send_f = total(own, arrived)
    recv_f = lax.all_to_all(send_f.reshape(groups_z, 4, columns), "gz", 0, 0, tiled=True)
    recv_f = recv_f.reshape(4 * columns, columns)
    up = [(i, i + 1) for i in range(groups_z - 1)]
    down = [(b, a) for a, b in up]
    edge_planes, _ = lax.optimization_barrier((stacked, send_f))
    before = lax.ppermute(edge_planes, "gz", up)
    after = lax.ppermute(edge_planes, "gz", down)
    tx_back, ny_back = halves(t["tx_back"]), halves(t["ny_back"])
    return finish(recv_f, arrived, stacked, before, after, tx_back, ny_back)[:, None]


def solution(mesh):
    placed = (
        P(None, ("parts", "gz"), "gy", None),
        P(("parts", "gz"), "gy", None),
        P(),
        P(None, "gz", "gy", None),
        P(None, "gz", "gy"),
    )

    return jax.shard_map(
        local,
        mesh=mesh,
        in_specs=placed,
        out_specs=P(None, ("parts", "gz"), "gy", None),
        check_vma=False,
    )
```

```python
import functools

import jax
import jax.numpy as jnp
import numpy as np
from jax import lax
from jax.experimental import pallas as pl
from jax.experimental.pallas import tpu as pltpu
from jax.sharding import PartitionSpec as P


exchange_stiffness = 0.25
tensor_index = ((0, 3, 4), (3, 1, 5), (4, 5, 2))
swap = [(0, 1), (1, 0)]
bf16 = jnp.bfloat16
f32 = jnp.float32
limits = pltpu.CompilerParams(vmem_limit_bytes=20 * 2**20)


def wave(first, second, period):
    angle = 2.0 * np.pi / period * (np.outer(first, second) % period)
    return np.cos(angle), np.sin(angle)


def slot_frequencies(groups_z):
    bits = groups_z.bit_length() - 1
    reversed_bits = np.array([int(format(d, f"0{bits}b")[::-1], 2) for d in range(groups_z)])
    return np.concatenate([2 * reversed_bits, 2 * reversed_bits + 1])


def tables(columns, rows, groups_z):
    half = rows // 2
    x = np.arange(columns)
    y = np.arange(rows)
    ky = np.arange(2 * rows)
    z = np.arange(groups_z)
    out = {}
    cx, sx = wave(x, x, 2 * columns)
    out["tx"] = np.concatenate([cx, -sx], axis=1)
    forward, back = [], []
    for g in range(2):
        own_ky = ky[g * rows : (g + 1) * rows]
        there, here = [], []
        for h in (g, 1 - g):
            c, s = wave(y[h * half : (h + 1) * half], own_ky, 2 * rows)
            there.append(np.block([[c, -s], [s, c]]))
            here.append(np.block([[c.T, s.T], [-s.T, c.T]]))
        forward.append(np.concatenate(there, axis=0))
        back.append(np.concatenate(here, axis=1))
    out["ty"] = np.stack(forward)
    out["ty_back"] = np.stack(back)
    c, s = wave(slot_frequencies(groups_z), z, 2 * groups_z)
    out["tz"] = np.concatenate([c, s], axis=1)
    out["tz_back"] = np.stack([np.concatenate([t[k * groups_z : (k + 1) * groups_z].T for t in (c, s)], axis=1) for k in range(2)])
    w = np.where(x == 0, 1.0, 2.0)[:, None]
    scale = 1.0 / (2.0 * columns * 2.0 * rows * 2.0 * groups_z)
    out["tx_back"] = np.concatenate([w * cx, -w * sx], axis=1) * scale
    forward, back = [], []
    for g in range(2):
        c, s = wave(ky, y[g * half : (g + 1) * half], 2 * rows)
        c, s = c.reshape(2, rows, half), s.reshape(2, rows, half)
        forward.append(np.concatenate([c[0], -s[0], c[1], -s[1]], axis=1))
        back.append(np.concatenate([c[0].T, -s[0].T, c[1].T, -s[1].T], axis=0) * scale)
    out["ny"] = np.stack(forward)
    out["ny_back"] = np.stack(back)
    return out


def halves(table):
    table = np.asarray(table, dtype=np.float32)
    high = table.astype(bf16)
    low = (table - high.astype(np.float32)).astype(bf16)
    return jnp.asarray(np.stack([high, low]))


def split(x):
    high = x.astype(bf16)
    return high, (x - high.astype(f32)).astype(bf16)


def three(left, right, dims=((1,), (0,))):
    (lh, ll), (rh, rl) = left, right
    prod = lambda a, b: lax.dot_general(a, b, (dims, ((), ())), preferred_element_type=f32)
    return prod(lh, rh) + (prod(lh, rl) + prod(ll, rh))


def cross(real, imag, lower):
    return jnp.concatenate([jnp.concatenate([real, imag], axis=1), lower], axis=0)


def place(axis, count):
    return lax.rem(lax.axis_index(axis), count)


def prepare_kernel(slots, sat_hbm, dir_hbm, reg_hbm, main_hbm, nyq_hbm, tx_hbm, ny_hbm,
                   send_ref, stack_ref, sat_ref, dirs, reg, main, nyq, tx, ny, rows_t, sems):
    _, half, columns = dirs.shape
    width = 4 + 6 * slots
    slot = place("parts", 2 // slots)
    copies = [
        pltpu.make_async_copy(reg_hbm, reg, sems.at[0]),
        pltpu.make_async_copy(dir_hbm, dirs, sems.at[1]),
        pltpu.make_async_copy(main_hbm.at[:, pl.ds(slot, slots)], main, sems.at[2]),
        pltpu.make_async_copy(tx_hbm, tx, sems.at[3]),
        pltpu.make_async_copy(ny_hbm.at[place("gy", 2)], ny, sems.at[4]),
        pltpu.make_async_copy(nyq_hbm, nyq, sems.at[5]),
        pltpu.make_async_copy(sat_hbm, sat_ref, sems.at[6]),
    ]
    for c in copies:
        c.start()
    rows_t[...] = jnp.zeros_like(rows_t)
    copies[0].wait()
    region = reg[...]
    magnetic = (region > 0).astype(f32)
    strength = jnp.zeros(region.shape, f32)
    copies[6].wait()
    for r in range(3):
        strength = strength + jnp.where(region == r + 1, sat_ref[r], 0.0)
    copies[1].wait()
    stack_ref[3] = magnetic
    lane = lax.broadcasted_iota(jnp.int32, (half, columns), 1)
    signs = (1 - 2 * (lane % 2)).astype(f32)
    moments = []
    sums = jnp.zeros((half, columns), f32)
    for c in range(3):
        one = dirs[c]
        stack_ref[c] = one * magnetic
        moment = one * strength
        moments.append(moment)
        total = jnp.sum(moment * signs, axis=1, keepdims=True)
        sums = jnp.where((lane % 4 == c) & (lane % 32 < 12), total, sums)
    copies[3].wait()
    zero = jnp.zeros((half, columns), bf16)
    table = (tx[0], tx[1])
    for c in range(3):
        high, low = split(moments[c])
        wide = [jnp.concatenate([jnp.concatenate([p, zero], 1), jnp.concatenate([zero, p], 1)], 0) for p in (high, low)]
        send_ref[pl.ds(c, columns, stride=width), :] = three(table, wide, ((1,), (1,)))
    copies[2].wait()
    for s in range(slots):
        for r in range(6):
            send_ref[pl.ds(4 + 6 * s + r, columns, stride=width), :] = main[r, s].T
    copies[4].wait()
    parts = [split(jnp.where(lane // 32 == q, sums, 0.0)) for q in range(4)]
    stacked = [jnp.concatenate([p[k] for p in parts], axis=0) for k in range(2)]
    row = three((ny[0], ny[1]), stacked)
    copies[5].wait()
    for s in range(2):
        for i in range(3):
            for j in range(3):
                rows_t[pl.ds(64 * s + 16 + 4 * i + j, 1), :] = nyq[tensor_index[i][j], pl.ds(s, 1), :]
    send_ref[pl.ds(3, columns, stride=width), :] = row + rows_t[...].T


def prepare(saturation, direction, region, kernel_main, kernel_nyq, tx, ny, slots):
    _, half, columns = direction.shape
    rows = kernel_main.shape[2]
    any_spec = pl.BlockSpec(memory_space=pltpu.HBM)
    vmem = pl.BlockSpec(memory_space=pltpu.VMEM)

    return pl.pallas_call(
        functools.partial(prepare_kernel, slots),
        name="prepare",
        compiler_params=limits,
        out_shape=(
            jax.ShapeDtypeStruct((columns * (4 + 6 * slots), columns), f32),
            jax.ShapeDtypeStruct((4, half, columns), f32),
        ),
        in_specs=[any_spec] * 7,
        out_specs=(vmem, vmem),
        scratch_shapes=[
            pltpu.SMEM(saturation.shape, f32),
            pltpu.VMEM((3, half, columns), f32),
            pltpu.VMEM((half, columns), jnp.int32),
            pltpu.VMEM((6, slots, rows, columns), f32),
            pltpu.VMEM(kernel_nyq.shape, f32),
            pltpu.VMEM(tx.shape, bf16),
            pltpu.VMEM(ny.shape[1:], bf16),
            pltpu.VMEM((columns, columns), f32),
            pltpu.SemaphoreType.DMA((7,)),
        ],
    )(*(pltpu.with_memory_space_constraint(a, pltpu.HBM) for a in (saturation, direction, region, kernel_main, kernel_nyq, tx, ny)))


def forward_kernel(own, other, ty, tz, out):
    planes, width = own.shape[1:]
    gy = place("gy", 2)
    table = (tz[0], tz[1])
    y_table = (ty[0, gy], ty[1, gy])
    for c in range(4):
        if c < 3:
            ready = three(split(jnp.concatenate([own[c], other[c]], axis=1)), y_table)
            real, imag = ready[:, :width], ready[:, width:]
        else:
            lane = lax.broadcasted_iota(jnp.int32, (planes, width), 1)
            summed = own[3] + other[3]
            summed = jnp.where(place("gy", 2) == 0, summed, pltpu.roll(summed, 64, 1))
            real = jnp.where(lane < 12, summed, 0.0)
            imag = jnp.where(lane < 12, pltpu.roll(summed, width - 32, 1), 0.0)
        (rh, rl), (ih, il) = split(real), split(imag)
        crossed = [cross(r, i, jnp.concatenate([i, -r], axis=1)) for r, i in ((rh, ih), (rl, il))]
        done = three(table, crossed)
        out[c, 0] = done[:planes]
        out[c, 1] = done[planes:]


def forward(own, other, ty, tz):
    planes, width = own.shape[1:]
    vmem = pl.BlockSpec(memory_space=pltpu.VMEM)
    return pl.pallas_call(
        forward_kernel,
        name="forward",
        compiler_params=limits,
        out_shape=jax.ShapeDtypeStruct((4, 2, planes, 2 * width), f32),
        in_specs=[vmem] * 4,
        out_specs=vmem,
    )(own, other, ty, tz)


def back(real, imag, table):
    (rh, rl), (ih, il) = split(real), split(imag)
    crossed = [cross(r, i, jnp.concatenate([-i, r], axis=1)) for r, i in ((rh, ih), (rl, il))]
    return three(table, crossed)


def field_of(kernel, spectra, slot, i):
    width = kernel.shape[2]
    real = imag = None
    for j in range(3):
        k = kernel[tensor_index[i][j]]
        a, b = k * spectra[j, slot, :, :width], k * spectra[j, slot, :, width:]
        real, imag = (a, b) if real is None else (real + a, imag + b)
    return real, imag


def first_half_kernel(pairs, spectra, kernel, row_ref, tz, out, line_out):
    planes, width = row_ref.shape
    slot = place("parts", pairs)
    table = (tz[0, slot], tz[1, slot])
    for i in range(3):
        out[i] = back(*field_of(kernel, spectra, slot, i), table)
    lane = lax.broadcasted_iota(jnp.int32, (planes, width), 1)
    row = row_ref[...]
    line = jnp.zeros((planes, 2 * width), f32)
    for s in range(2):
        k = jnp.where(lane < 12, pltpu.roll(row, width - 16 - 64 * s, 1), 0.0)
        line = line + back(spectra[3, s, :, :width] * k, spectra[3, s, :, width:] * k, (tz[0, s], tz[1, s]))
    line = line[:, :width] + pltpu.roll(line[:, width:], 32, 1)
    line_out[...] = jnp.where(place("gy", 2) == 0, line, pltpu.roll(line, 64, 1))


def first_half(pairs, spectra, kernel, row, tz):
    planes, width = row.shape
    vmem = pl.BlockSpec(memory_space=pltpu.VMEM)
    return pl.pallas_call(
        functools.partial(first_half_kernel, pairs),
        name="first_half",
        compiler_params=limits,
        out_shape=(
            jax.ShapeDtypeStruct((3, planes, 2 * width), f32),
            jax.ShapeDtypeStruct((planes, width), f32),
        ),
        in_specs=[vmem] * 4,
        out_specs=(vmem, vmem),
    )(spectra, kernel, row, tz)


def second_half_kernel(pairs, spectra, kernel, ready, line_ref, stack, tz, ty, lines_out, other):
    planes, width = line_ref.shape
    slot = 1 - place("parts", pairs)
    gy = place("gy", 2)
    table = (tz[0, slot], tz[1, slot])
    y_table = (ty[0, gy, :, width:], ty[1, gy, :, width:])
    for i in range(3):
        lines = ready[i] + back(*field_of(kernel, spectra, slot, i), table)
        lines_out[i] = lines
        other[pl.ds(i, planes, stride=4), :] = three(split(lines), y_table)
    other[pl.ds(3, planes, stride=4), :] = line_ref[...]
    last = stack.shape[1] - 1
    for c in range(4):
        edge = jnp.where(gy == 0, stack[c, last:], stack[c, :1])
        other[4 * planes + c : 4 * planes + c + 1, :] = edge
        other[4 * planes + 4 + c : 4 * planes + 5 + c, :] = edge


def second_half(pairs, spectra, kernel, ready, line, stacked, tz, ty):
    planes, width = line.shape
    vmem = pl.BlockSpec(memory_space=pltpu.VMEM)
    return pl.pallas_call(
        functools.partial(second_half_kernel, pairs),
        name="second_half",
        compiler_params=limits,
        out_shape=(
            jax.ShapeDtypeStruct((3, planes, 2 * width), f32),
            jax.ShapeDtypeStruct((4 * planes + 8, width), f32),
        ),
        in_specs=[vmem] * 7,
        out_specs=(vmem, vmem),
    )(spectra, kernel, ready, line, stacked, tz, ty)


def own_half_kernel(lines, line_ref, ty, own):
    planes, width = line_ref.shape
    gy = place("gy", 2)
    y_table = (ty[0, gy, :, :width], ty[1, gy, :, :width])
    for i in range(3):
        own[pl.ds(i, planes, stride=4), :] = three(split(lines[i]), y_table)
    own[pl.ds(3, planes, stride=4), :] = line_ref[...]


def own_half(lines, line, ty):
    planes, width = line.shape
    vmem = pl.BlockSpec(memory_space=pltpu.VMEM)
    return pl.pallas_call(
        own_half_kernel,
        name="own_half",
        compiler_params=limits,
        out_shape=jax.ShapeDtypeStruct((4 * planes, width), f32),
        in_specs=[vmem] * 3,
        out_specs=vmem,
    )(lines, line, ty)


def exchange_kernel(arrived, stack, before, after, out):
    _, half, columns = stack.shape
    lane = lax.broadcasted_iota(jnp.int32, (half, columns), 1)
    line = lax.broadcasted_iota(jnp.int32, (half, columns), 0)
    lower = place("gy", 2) == 0
    first_edge = arrived.shape[0] - 8

    def near(c):
        one = stack[c]
        edge = arrived[pl.ds(first_edge + c, 1), :]
        low = jnp.where(line == 0, jnp.where(lower, 0.0, edge), pltpu.roll(one, 1, 0))
        high = jnp.where(line == half - 1, jnp.where(lower, edge, 0.0), pltpu.roll(one, half - 1, 0))
        left = jnp.where(lane == 0, 0.0, pltpu.roll(one, 1, 1))
        right = jnp.where(lane == columns - 1, 0.0, pltpu.roll(one, columns - 1, 1))
        return before[c] + after[c] + low + high + left + right

    count = near(3)
    magnetic = stack[3]
    for c in range(3):
        out[c] = exchange_stiffness * (magnetic * near(c) - count * stack[c])


def exchange(arrived, stacked, before, after):
    vmem = pl.BlockSpec(memory_space=pltpu.VMEM)
    return pl.pallas_call(
        exchange_kernel,
        name="exchange",
        compiler_params=limits,
        out_shape=jax.ShapeDtypeStruct((3,) + stacked.shape[1:], f32),
        in_specs=[vmem] * 4,
        out_specs=vmem,
    )(arrived, stacked, before, after)


def finish_kernel(recv, added, tx, ny, out):
    _, half, columns = added.shape
    lane = lax.broadcasted_iota(jnp.int32, (half, columns), 1)
    signs = (1 - 2 * (lane % 2)).astype(f32)
    gy = place("gy", 2)
    nyquist = three((ny[0, gy], ny[1, gy]), split(recv[pl.ds(3, columns, stride=4), :]))
    sums = jnp.zeros((half, columns), f32)
    for q in range(4):
        sums = jnp.where(lane // 32 == q, nyquist[q * half : (q + 1) * half], sums)
    table = (tx[0], tx[1])
    for c in range(3):
        prod = three(split(recv[pl.ds(c, columns, stride=4), :].T), table)
        demag = prod[:half, :columns] + prod[half:, columns:]
        total = jnp.sum(jnp.where(lane % 32 // 4 == c, sums, 0.0), axis=1, keepdims=True)
        out[c] = demag + total * signs + added[c]


def finish(recv, added, tx, ny):
    vmem = pl.BlockSpec(memory_space=pltpu.VMEM)
    return pl.pallas_call(
        finish_kernel,
        name="finish",
        compiler_params=limits,
        out_shape=jax.ShapeDtypeStruct(added.shape, f32),
        in_specs=[vmem] * 4,
        out_specs=vmem,
    )(recv, added, tx, ny)


def local(direction, region, saturation, kernel_main, kernel_nyq):
    columns = direction.shape[3]
    half = direction.shape[2]
    groups_z = lax.axis_size("gz")
    rows = half * lax.axis_size("gy")
    parts = lax.axis_size("parts")
    pairs = 2 if parts % 2 == 0 else 1
    slots = 2 // pairs
    t = tables(columns, rows, groups_z)
    direction = direction[:, 0]
    send, stacked = prepare(
        saturation, direction, region[0], kernel_main, kernel_nyq,
        halves(t["tx"]), halves(t["ny"]).swapaxes(0, 1), slots,
    )
    width = 4 + 6 * slots
    recv = lax.all_to_all(send.reshape(columns, width // 2, 2, columns), "gz", 0, 0, tiled=True)
    recv = recv.reshape(columns, width, columns).transpose(1, 0, 2)
    kernel = recv[4:10]
    if pairs == 2:
        kernel_other = lax.ppermute(kernel, "parts", [(p, p ^ 1) for p in range(parts)])
    else:
        kernel_other = recv[10:]
    own_m = recv[:4]
    other_m = lax.ppermute(own_m, "gy", swap)
    tz_back = halves(t["tz_back"])
    spectra = forward(own_m, other_m, halves(t["ty"]), halves(t["tz"]))
    ready, line = first_half(pairs, spectra, kernel, own_m[3], tz_back)
    ty_back = halves(t["ty_back"])
    lines, other = second_half(pairs, spectra, kernel_other, ready, line, stacked, tz_back, ty_back)
    arrived = lax.ppermute(other, "gy", swap)
    own = own_half(lines, line, ty_back)
    send_f = own + arrived[: 4 * groups_z]
    recv_f = lax.all_to_all(send_f.reshape(groups_z, 4, columns), "gz", 0, 0, tiled=True)
    recv_f = recv_f.reshape(4 * columns, columns)
    up = [(i, i + 1) for i in range(groups_z - 1)]
    down = [(b, a) for a, b in up]
    edge_planes, _ = lax.optimization_barrier((stacked, send_f))
    before = lax.ppermute(edge_planes, "gz", up)
    after = lax.ppermute(edge_planes, "gz", down)
    tx_back, ny_back = halves(t["tx_back"]), halves(t["ny_back"])
    return finish(recv_f, exchange(arrived, stacked, before, after), tx_back, ny_back)[:, None]


def solution(mesh):
    placed = (
        P(None, ("parts", "gz"), "gy", None),
        P(("parts", "gz"), "gy", None),
        P(),
        P(None, "gz", "gy", None),
        P(None, "gz", "gy"),
    )

    return jax.shard_map(
        local,
        mesh=mesh,
        in_specs=placed,
        out_specs=P(None, ("parts", "gz"), "gy", None),
        check_vma=False,
    )
```

```python
import functools

import jax
import jax.numpy as jnp
import numpy as np
from jax import lax
from jax.experimental import pallas as pl
from jax.experimental.pallas import tpu as pltpu
from jax.sharding import PartitionSpec as P


exchange_stiffness = 0.25
tensor_index = ((0, 3, 4), (3, 1, 5), (4, 5, 2))
swap = [(0, 1), (1, 0)]
bf16 = jnp.bfloat16
f32 = jnp.float32
limits = pltpu.CompilerParams(vmem_limit_bytes=20 * 2**20)


def wave(first, second, period):
    angle = 2.0 * np.pi / period * (np.outer(first, second) % period)
    return np.cos(angle), np.sin(angle)


def slot_frequencies(groups_z):
    bits = groups_z.bit_length() - 1
    reversed_bits = np.array([int(format(d, f"0{bits}b")[::-1], 2) for d in range(groups_z)])
    return np.concatenate([2 * reversed_bits, 2 * reversed_bits + 1])


def tables(columns, rows, groups_z):
    half = rows // 2
    x = np.arange(columns)
    y = np.arange(rows)
    ky = np.arange(2 * rows)
    z = np.arange(groups_z)
    out = {}
    cx, sx = wave(x, x, 2 * columns)
    out["tx"] = np.concatenate([cx, -sx], axis=1)
    forward, back = [], []
    for g in range(2):
        own_ky = ky[g * rows : (g + 1) * rows]
        there, here = [], []
        for h in (g, 1 - g):
            c, s = wave(y[h * half : (h + 1) * half], own_ky, 2 * rows)
            there.append(np.block([[c, -s], [s, c]]))
            here.append(np.block([[c.T, s.T], [-s.T, c.T]]))
        forward.append(np.concatenate(there, axis=0))
        back.append(np.concatenate(here, axis=1))
    out["ty"] = np.stack(forward)
    out["ty_back"] = np.stack(back)
    c, s = wave(slot_frequencies(groups_z), z, 2 * groups_z)
    out["tz"] = np.concatenate([c, s], axis=1)
    out["tz_back"] = np.stack([np.concatenate([t[k * groups_z : (k + 1) * groups_z].T for t in (c, s)], axis=1) for k in range(2)])
    w = np.where(x == 0, 1.0, 2.0)[:, None]
    scale = 1.0 / (2.0 * columns * 2.0 * rows * 2.0 * groups_z)
    out["tx_back"] = np.concatenate([w * cx, -w * sx], axis=1) * scale
    forward, back = [], []
    for g in range(2):
        c, s = wave(ky, y[g * half : (g + 1) * half], 2 * rows)
        c, s = c.reshape(2, rows, half), s.reshape(2, rows, half)
        forward.append(np.concatenate([c[0], -s[0], c[1], -s[1]], axis=1))
        back.append(np.concatenate([c[0].T, -s[0].T, c[1].T, -s[1].T], axis=0) * scale)
    out["ny"] = np.stack(forward)
    out["ny_back"] = np.stack(back)
    return out


def halves(table):
    table = np.asarray(table, dtype=np.float32)
    high = table.astype(bf16)
    low = (table - high.astype(np.float32)).astype(bf16)
    return jnp.asarray(np.stack([high, low]))


def split(x):
    high = x.astype(bf16)
    return high, (x - high.astype(f32)).astype(bf16)


def three(left, right, dims=((1,), (0,))):
    (lh, ll), (rh, rl) = left, right
    prod = lambda a, b: lax.dot_general(a, b, (dims, ((), ())), preferred_element_type=f32)
    return prod(lh, rh) + (prod(lh, rl) + prod(ll, rh))


def cross(real, imag, lower):
    return jnp.concatenate([jnp.concatenate([real, imag], axis=1), lower], axis=0)


def place(axis, count):
    return lax.rem(lax.axis_index(axis), count)


def prepare_kernel(slots, sat_hbm, dir_hbm, reg_hbm, main_hbm, nyq_hbm, tx_hbm, ny_hbm,
                   send_ref, stack_ref, sat_ref, dirs, reg, main, nyq, tx, ny, rows_t, sems):
    _, half, columns = dirs.shape
    width = 4 + 6 * slots
    slot = place("parts", 2 // slots)
    copies = [
        pltpu.make_async_copy(reg_hbm, reg, sems.at[0]),
        pltpu.make_async_copy(dir_hbm, dirs, sems.at[1]),
        pltpu.make_async_copy(main_hbm.at[:, pl.ds(slot, slots)], main, sems.at[2]),
        pltpu.make_async_copy(tx_hbm, tx, sems.at[3]),
        pltpu.make_async_copy(ny_hbm.at[place("gy", 2)], ny, sems.at[4]),
        pltpu.make_async_copy(nyq_hbm, nyq, sems.at[5]),
        pltpu.make_async_copy(sat_hbm, sat_ref, sems.at[6]),
    ]
    for k in (6, 0, 1, 3, 2, 4, 5):
        copies[k].start()
    rows_t[...] = jnp.zeros_like(rows_t)
    copies[0].wait()
    region = reg[...]
    magnetic = (region > 0).astype(f32)
    strength = jnp.zeros(region.shape, f32)
    copies[6].wait()
    for r in range(3):
        strength = strength + jnp.where(region == r + 1, sat_ref[r], 0.0)
    copies[1].wait()
    stack_ref[3] = magnetic
    lane = lax.broadcasted_iota(jnp.int32, (half, columns), 1)
    signs = (1 - 2 * (lane % 2)).astype(f32)
    moments = []
    sums = jnp.zeros((half, columns), f32)
    for c in range(3):
        one = dirs[c]
        stack_ref[c] = one * magnetic
        moment = one * strength
        moments.append(moment)
        total = jnp.sum(moment * signs, axis=1, keepdims=True)
        sums = jnp.where((lane % 4 == c) & (lane % 32 < 12), total, sums)
    copies[3].wait()
    zero = jnp.zeros((half, columns), bf16)
    table = (tx[0], tx[1])
    for c in range(3):
        high, low = split(moments[c])
        wide = [jnp.concatenate([jnp.concatenate([p, zero], 1), jnp.concatenate([zero, p], 1)], 0) for p in (high, low)]
        send_ref[pl.ds(c, columns, stride=width), :] = three(table, wide, ((1,), (1,)))
    copies[2].wait()
    for s in range(slots):
        for r in range(6):
            send_ref[pl.ds(4 + 6 * s + r, columns, stride=width), :] = main[r, s].T
    copies[4].wait()
    parts = [split(jnp.where(lane // 32 == q, sums, 0.0)) for q in range(4)]
    stacked = [jnp.concatenate([p[k] for p in parts], axis=0) for k in range(2)]
    row = three((ny[0], ny[1]), stacked)
    copies[5].wait()
    for s in range(2):
        for i in range(3):
            for j in range(3):
                rows_t[pl.ds(64 * s + 16 + 4 * i + j, 1), :] = nyq[tensor_index[i][j], pl.ds(s, 1), :]
    send_ref[pl.ds(3, columns, stride=width), :] = row + rows_t[...].T


def prepare(saturation, direction, region, kernel_main, kernel_nyq, tx, ny, slots):
    _, half, columns = direction.shape
    rows = kernel_main.shape[2]
    any_spec = pl.BlockSpec(memory_space=pltpu.HBM)
    vmem = pl.BlockSpec(memory_space=pltpu.VMEM)

    return pl.pallas_call(
        functools.partial(prepare_kernel, slots),
        name="prepare",
        compiler_params=limits,
        out_shape=(
            jax.ShapeDtypeStruct((columns * (4 + 6 * slots), columns), f32),
            jax.ShapeDtypeStruct((4, half, columns), f32),
        ),
        in_specs=[any_spec] * 7,
        out_specs=(vmem, vmem),
        scratch_shapes=[
            pltpu.SMEM(saturation.shape, f32),
            pltpu.VMEM((3, half, columns), f32),
            pltpu.VMEM((half, columns), jnp.int32),
            pltpu.VMEM((6, slots, rows, columns), f32),
            pltpu.VMEM(kernel_nyq.shape, f32),
            pltpu.VMEM(tx.shape, bf16),
            pltpu.VMEM(ny.shape[1:], bf16),
            pltpu.VMEM((columns, columns), f32),
            pltpu.SemaphoreType.DMA((7,)),
        ],
    )(*(pltpu.with_memory_space_constraint(a, pltpu.HBM) for a in (saturation, direction, region, kernel_main, kernel_nyq, tx, ny)))


def forward_kernel(own, other, ty, tz, out):
    planes, width = own.shape[1:]
    gy = place("gy", 2)
    table = (tz[0], tz[1])
    y_table = (ty[0, gy], ty[1, gy])
    for c in range(4):
        if c < 3:
            ready = three(split(jnp.concatenate([own[c], other[c]], axis=1)), y_table)
            real, imag = ready[:, :width], ready[:, width:]
        else:
            lane = lax.broadcasted_iota(jnp.int32, (planes, width), 1)
            summed = own[3] + other[3]
            summed = jnp.where(place("gy", 2) == 0, summed, pltpu.roll(summed, 64, 1))
            real = jnp.where(lane < 12, summed, 0.0)
            imag = jnp.where(lane < 12, pltpu.roll(summed, width - 32, 1), 0.0)
        (rh, rl), (ih, il) = split(real), split(imag)
        crossed = [cross(r, i, jnp.concatenate([i, -r], axis=1)) for r, i in ((rh, ih), (rl, il))]
        done = three(table, crossed)
        out[c, 0] = done[:planes]
        out[c, 1] = done[planes:]


def forward(own, other, ty, tz):
    planes, width = own.shape[1:]
    vmem = pl.BlockSpec(memory_space=pltpu.VMEM)
    return pl.pallas_call(
        forward_kernel,
        name="forward",
        compiler_params=limits,
        out_shape=jax.ShapeDtypeStruct((4, 2, planes, 2 * width), f32),
        in_specs=[vmem] * 4,
        out_specs=vmem,
    )(own, other, ty, tz)


def back(real, imag, table):
    (rh, rl), (ih, il) = split(real), split(imag)
    crossed = [cross(r, i, jnp.concatenate([-i, r], axis=1)) for r, i in ((rh, ih), (rl, il))]
    return three(table, crossed)


def field_of(kernel, spectra, slot, i):
    width = kernel.shape[2]
    real = imag = None
    for j in range(3):
        k = kernel[tensor_index[i][j]]
        a, b = k * spectra[j, slot, :, :width], k * spectra[j, slot, :, width:]
        real, imag = (a, b) if real is None else (real + a, imag + b)
    return real, imag


def first_half_kernel(pairs, spectra, kernel, row_ref, tz, out, line_out):
    planes, width = row_ref.shape
    slot = place("parts", pairs)
    table = (tz[0, slot], tz[1, slot])
    for i in range(3):
        out[i] = back(*field_of(kernel, spectra, slot, i), table)
    lane = lax.broadcasted_iota(jnp.int32, (planes, width), 1)
    row = row_ref[...]
    line = jnp.zeros((planes, 2 * width), f32)
    for s in range(2):
        k = jnp.where(lane < 12, pltpu.roll(row, width - 16 - 64 * s, 1), 0.0)
        line = line + back(spectra[3, s, :, :width] * k, spectra[3, s, :, width:] * k, (tz[0, s], tz[1, s]))
    line = line[:, :width] + pltpu.roll(line[:, width:], 32, 1)
    line_out[...] = jnp.where(place("gy", 2) == 0, line, pltpu.roll(line, 64, 1))


def first_half(pairs, spectra, kernel, row, tz):
    planes, width = row.shape
    vmem = pl.BlockSpec(memory_space=pltpu.VMEM)
    return pl.pallas_call(
        functools.partial(first_half_kernel, pairs),
        name="first_half",
        compiler_params=limits,
        out_shape=(
            jax.ShapeDtypeStruct((3, planes, 2 * width), f32),
            jax.ShapeDtypeStruct((planes, width), f32),
        ),
        in_specs=[vmem] * 4,
        out_specs=(vmem, vmem),
    )(spectra, kernel, row, tz)


def second_half_kernel(pairs, spectra, kernel, ready, line_ref, stack, tz, ty, own, other):
    planes, width = line_ref.shape
    slot = 1 - place("parts", pairs)
    gy = place("gy", 2)
    table = (tz[0, slot], tz[1, slot])
    y_table = (ty[0, gy], ty[1, gy])
    for i in range(3):
        lines = ready[i] + back(*field_of(kernel, spectra, slot, i), table)
        lines = three(split(lines), y_table)
        own[pl.ds(i, planes, stride=4), :] = lines[:, :width]
        other[pl.ds(i, planes, stride=4), :] = lines[:, width:]
    own[pl.ds(3, planes, stride=4), :] = line_ref[...]
    other[pl.ds(3, planes, stride=4), :] = line_ref[...]
    last = stack.shape[1] - 1
    for c in range(4):
        edge = jnp.where(place("gy", 2) == 0, stack[c, last:], stack[c, :1])
        other[4 * planes + c : 4 * planes + c + 1, :] = edge
        other[4 * planes + 4 + c : 4 * planes + 5 + c, :] = edge


def second_half(pairs, spectra, kernel, ready, line, stacked, tz, ty):
    planes, width = line.shape
    vmem = pl.BlockSpec(memory_space=pltpu.VMEM)
    return pl.pallas_call(
        functools.partial(second_half_kernel, pairs),
        name="second_half",
        compiler_params=limits,
        out_shape=(
            jax.ShapeDtypeStruct((4 * planes, width), f32),
            jax.ShapeDtypeStruct((4 * planes + 8, width), f32),
        ),
        in_specs=[vmem] * 7,
        out_specs=(vmem, vmem),
    )(spectra, kernel, ready, line, stacked, tz, ty)


def finish_kernel(recv, arrived, stack, before, after, tx, ny, out):
    _, half, columns = stack.shape
    lane = lax.broadcasted_iota(jnp.int32, (half, columns), 1)
    line = lax.broadcasted_iota(jnp.int32, (half, columns), 0)
    signs = (1 - 2 * (lane % 2)).astype(f32)
    gy = place("gy", 2)
    lower = gy == 0

    def near(c):
        one = stack[c]
        edge = arrived[pl.ds(4 * columns + c, 1), :]
        low = jnp.where(line == 0, jnp.where(lower, 0.0, edge), pltpu.roll(one, 1, 0))
        high = jnp.where(line == half - 1, jnp.where(lower, edge, 0.0), pltpu.roll(one, half - 1, 0))
        left = jnp.where(lane == 0, 0.0, pltpu.roll(one, 1, 1))
        right = jnp.where(lane == columns - 1, 0.0, pltpu.roll(one, columns - 1, 1))
        return before[c] + after[c] + low + high + left + right

    count = near(3)
    magnetic = stack[3]
    nyquist = three((ny[0, gy], ny[1, gy]), split(recv[pl.ds(3, columns, stride=4), :]))
    sums = jnp.zeros((half, columns), f32)
    for q in range(4):
        sums = jnp.where(lane // 32 == q, nyquist[q * half : (q + 1) * half], sums)
    table = (tx[0], tx[1])
    for c in range(3):
        prod = three(split(recv[pl.ds(c, columns, stride=4), :].T), table)
        demag = prod[:half, :columns] + prod[half:, columns:]
        total = jnp.sum(jnp.where(lane % 32 // 4 == c, sums, 0.0), axis=1, keepdims=True)
        exchange = exchange_stiffness * (magnetic * near(c) - count * stack[c])
        out[c] = demag + total * signs + exchange


def finish(recv, arrived, stacked, before, after, tx, ny):
    vmem = pl.BlockSpec(memory_space=pltpu.VMEM)
    return pl.pallas_call(
        finish_kernel,
        name="finish",
        compiler_params=limits,
        out_shape=jax.ShapeDtypeStruct((3,) + stacked.shape[1:], f32),
        in_specs=[vmem] * 7,
        out_specs=vmem,
    )(recv, arrived, stacked, before, after, tx, ny)


def local(direction, region, saturation, kernel_main, kernel_nyq):
    columns = direction.shape[3]
    half = direction.shape[2]
    groups_z = lax.axis_size("gz")
    rows = half * lax.axis_size("gy")
    parts = lax.axis_size("parts")
    pairs = 2 if parts % 2 == 0 else 1
    slots = 2 // pairs
    t = tables(columns, rows, groups_z)
    direction = direction[:, 0]
    send, stacked = prepare(
        saturation, direction, region[0], kernel_main, kernel_nyq,
        halves(t["tx"]), halves(t["ny"]).swapaxes(0, 1), slots,
    )
    width = 4 + 6 * slots
    recv = lax.all_to_all(send.reshape(columns, width // 2, 2, columns), "gz", 0, 0, tiled=True)
    recv = recv.reshape(columns, width, columns).transpose(1, 0, 2)
    kernel = recv[4:10]
    if pairs == 2:
        kernel_other = lax.ppermute(kernel, "parts", [(p, p ^ 1) for p in range(parts)])
    else:
        kernel_other = recv[10:]
    own_m = recv[:4]
    other_m = lax.ppermute(own_m, "gy", swap)
    tz_back = halves(t["tz_back"])
    spectra = forward(own_m, other_m, halves(t["ty"]), halves(t["tz"]))
    ready, line = first_half(pairs, spectra, kernel, own_m[3], tz_back)
    own, other = second_half(pairs, spectra, kernel_other, ready, line, stacked, tz_back, halves(t["ty_back"]))
    arrived = lax.ppermute(other, "gy", swap)
    send_f = own + arrived[: 4 * groups_z]
    recv_f = lax.all_to_all(send_f.reshape(groups_z, 4, columns), "gz", 0, 0, tiled=True)
    recv_f = recv_f.reshape(4 * columns, columns)
    up = [(i, i + 1) for i in range(groups_z - 1)]
    down = [(b, a) for a, b in up]
    edge_planes, _ = lax.optimization_barrier((stacked, send_f))
    before = lax.ppermute(edge_planes, "gz", up)
    after = lax.ppermute(edge_planes, "gz", down)
    tx_back, ny_back = halves(t["tx_back"]), halves(t["ny_back"])
    return finish(recv_f, arrived, stacked, before, after, tx_back, ny_back)[:, None]


def solution(mesh):
    placed = (
        P(None, ("parts", "gz"), "gy", None),
        P(("parts", "gz"), "gy", None),
        P(),
        P(None, "gz", "gy", None),
        P(None, "gz", "gy"),
    )

    return jax.shard_map(
        local,
        mesh=mesh,
        in_specs=placed,
        out_specs=P(None, ("parts", "gz"), "gy", None),
        check_vma=False,
    )
```
